32 devices in a mesh: dp: 2 (over x), etp: 4 (over z), ep: 4 (over y, core).
Axes of the slice: x: 2, y: 2, z: 4, core: 2. Of those that a mesh axis runs over, the one named last changes fastest.
Arguments:
- u_rows: bfloat16 [6144, 1536], P(('dp', 'ep', 'etp')), parts along dimension 0
- dy_rows: bfloat16 [6144, 1536], P(('dp', 'ep', 'etp')), parts along dimension 0
- topk_ids: int32 [6144, 4], P(('dp', 'ep', 'etp')), parts along dimension 0
- w_router: bfloat16 [1536, 32], replicated
- w_gate: bfloat16 [32, 1536, 768], P('ep', None, 'etp')
- w_up: bfloat16 [32, 1536, 768], P('ep', None, 'etp')
- w_down: bfloat16 [32, 768, 1536], P('ep', 'etp')
Outputs:
- output 1: bfloat16 [6144, 1536], P(('dp', 'ep', 'etp')), parts along dimension 0
- output 2: bfloat16 [6144, 1536], P(('dp', 'ep', 'etp')), parts along dimension 0
- output 3: float32 [64, 1536, 768], P(('dp', 'ep'), None, 'etp'), parts along dimension 0
- output 4: float32 [64, 1536, 768], P(('dp', 'ep'), None, 'etp'), parts along dimension 0
- output 5: float32 [64, 768, 1536], P(('dp', 'ep'), 'etp'), parts along dimension 0
- output 6: float32 [3072, 32], P('dp'), parts along dimension 0
There are 2 independent parts. The reference program is written for one: setup_inputs(seed, part) draws one part's arguments, and reference() takes and returns one part's arrays. A program takes and returns all parts, laid end to end along the dimension named above; an argument that names none is the same for every part.
All inputs are finite; a program needn't handle non-finite values.
Results may differ from the reference program's by a relative error of at most 0.0112347.
Values are sent between devices in bfloat16 or wider.
A program may use at most 1 GiB of HBM per device.

```python
import jax
import jax.numpy as jnp
from jax import lax

TOK_DEV = 192
SHARDS = 16
D_MODEL = 1536
EXPERTS = 32
TOP_K = 4
FFN = 768
TOKENS = TOK_DEV * SHARDS
CAP = min(TOK_DEV, (4 * TOK_DEV * TOP_K + EXPERTS - 1) // EXPERTS)
EXP_ROWS = SHARDS * CAP


def shard_ids(shard_key):
    key_perm, key_rank = jax.random.split(shard_key)
    expert_perm = jax.random.permutation(key_perm, EXPERTS)
    tok_rank = jax.random.permutation(key_rank, TOK_DEV)
    hot_expert = expert_perm[EXPERTS - 1]
    slot_col = jnp.arange(TOP_K)[None, :]
    has_hot = (tok_rank < CAP)[:, None]
    base_pos = tok_rank * TOP_K - jnp.minimum(tok_rank, CAP)
    cyc_pos = (base_pos[:, None] + slot_col - has_hot.astype(jnp.int32)) % (EXPERTS - 1)
    chosen = jnp.where(has_hot & (slot_col == 0), hot_expert, expert_perm[cyc_pos])
    return chosen.astype(jnp.int32)


def setup_inputs(seed: int = 0, part: int = 0) -> dict:
    part_key = jax.random.fold_in(jax.random.key(seed), part)
    key_tok, key_cot, key_route = jax.random.split(part_key, 3)
    key_router, key_gate, key_up, key_down = jax.random.split(jax.random.key(seed + 1), 4)
    topk_ids = jax.vmap(shard_ids)(jax.random.split(key_route, SHARDS)).reshape(TOKENS, TOP_K)
    u_rows = jax.random.normal(key_tok, (TOKENS, D_MODEL), jnp.float32).astype(jnp.bfloat16)
    dy_rows = jax.random.normal(key_cot, (TOKENS, D_MODEL), jnp.float32).astype(jnp.bfloat16)
    w_router = (jax.random.normal(key_router, (D_MODEL, EXPERTS), jnp.float32) * D_MODEL ** -0.5).astype(jnp.bfloat16)
    w_gate = (jax.random.normal(key_gate, (EXPERTS, D_MODEL, FFN), jnp.float32) * D_MODEL ** -0.5).astype(jnp.bfloat16)
    w_up = (jax.random.normal(key_up, (EXPERTS, D_MODEL, FFN), jnp.float32) * D_MODEL ** -0.5).astype(jnp.bfloat16)
    down_scale = 4.0 * EXPERTS / TOP_K * FFN ** -0.5
    w_down = (jax.random.normal(key_down, (EXPERTS, FFN, D_MODEL), jnp.float32) * down_scale).astype(jnp.bfloat16)
    return {"u_rows": u_rows, "dy_rows": dy_rows, "topk_ids": topk_ids, "w_router": w_router, "w_gate": w_gate, "w_up": w_up, "w_down": w_down}


def one_expert(u_wide, tok_rows, gate_rows, gate_e, up_e, down_e):
    x_rows = u_wide[tok_rows]
    h_gate = jnp.dot(x_rows, gate_e, preferred_element_type=jnp.float32).astype(jnp.bfloat16).astype(jnp.float32)
    h_up = jnp.dot(x_rows, up_e, preferred_element_type=jnp.float32).astype(jnp.bfloat16).astype(jnp.float32)
    act_rows = (jax.nn.silu(h_gate) * h_up).astype(jnp.bfloat16).astype(jnp.float32)
    out_rows = jnp.dot(act_rows, down_e, preferred_element_type=jnp.float32).astype(jnp.bfloat16).astype(jnp.float32)
    return gate_rows[:, None] * out_rows


def moe_forward(u_wide, topk_ids, router_wide, gate_wide, up_wide, down_wide):
    logits = jnp.dot(u_wide, router_wide, preferred_element_type=jnp.float32)
    router_prob = jax.nn.softmax(logits, axis=-1)
    gate_vals = jnp.take_along_axis(router_prob, topk_ids, axis=1).reshape(-1)
    flat_ids = topk_ids.reshape(-1)
    pair_order = jnp.argsort(flat_ids, stable=True)
    counts = jnp.bincount(flat_ids, length=EXPERTS)
    starts = jnp.cumsum(counts) - counts
    row_pos = jnp.arange(EXP_ROWS)
    is_valid = row_pos[None, :] < counts[:, None]
    pair_idx = pair_order[jnp.minimum(starts[:, None] + row_pos[None, :], TOKENS * TOP_K - 1)]
    tok_idx = pair_idx // TOP_K
    row_gate = jnp.where(is_valid, gate_vals[pair_idx], 0.0)
    expert_fn = jax.checkpoint(one_expert)

    def expert_step(moe_sum, per_expert):
        tok_rows, gate_rows, gate_e, up_e, down_e = per_expert
        contrib = expert_fn(u_wide, tok_rows, gate_rows, gate_e, up_e, down_e)
        return moe_sum.at[tok_rows].add(contrib), None

    moe_sum, unused = lax.scan(expert_step, jnp.zeros((TOKENS, D_MODEL), jnp.float32), (tok_idx, row_gate, gate_wide, up_wide, down_wide))
    return (u_wide + moe_sum).astype(jnp.bfloat16)


def reference(u_rows, dy_rows, topk_ids, w_router, w_gate, w_up, w_down):
    def forward(u_wide, router_wide, gate_wide, up_wide, down_wide):
        return moe_forward(u_wide, topk_ids, router_wide, gate_wide, up_wide, down_wide)

    y_rows, pull_back = jax.vjp(forward, u_rows.astype(jnp.float32), w_router.astype(jnp.float32), w_gate.astype(jnp.float32), w_up.astype(jnp.float32), w_down.astype(jnp.float32))
    du_wide, dw_router, dw_gate, dw_up, dw_down = pull_back(dy_rows)
    return y_rows, du_wide.astype(jnp.bfloat16), dw_gate, dw_up, dw_down, dw_router
```

```python
import jax
import jax.numpy as jnp
from jax import lax
from jax.experimental import pallas as pl
from jax.experimental.pallas import tpu as pltpu
from jax.sharding import PartitionSpec as P

MESH = pl.DeviceIdType.MESH
F32 = jnp.float32
BF16 = jnp.bfloat16
LANES = 256
LEVEL_ROWS = 32
HALF = 8
CHUNK = 512


def dot_nn(a, b):
    return lax.dot_general(a, b, (((1,), (0,)), ((), ())), preferred_element_type=F32)


def dot_nt(a, b):
    return lax.dot_general(a, b, (((1,), (1,)), ((), ())), preferred_element_type=F32)


def dot_tn(a, b):
    return lax.dot_general(a, b, (((0,), (0,)), ((), ())), preferred_element_type=F32)


def position():
    ep = lax.axis_index("ep")
    z = lax.axis_index("etp")
    return ep // 2, ep % 2, z


def block_of(y, c, z):
    return (y * 2 + c) * 4 + z


def near_order(z, q):
    near = z - 1 + 2 * (1 - jnp.minimum(z, 1))
    far = 3 * (1 - z // 2)
    third = 6 - z - near - far
    return jnp.where(q == 0, z, jnp.where(q == 1, near, jnp.where(q == 2, third, far)))


def far_order(z, k):
    first = 3 * (1 - z // 2)
    second = (2 + 3 * z) % 5
    third = 1 + z % 2
    return jnp.where(k == 0, first, jnp.where(k == 1, second, jnp.where(k == 2, third, z)))


def one_hot_slots(rank, cap):
    tok = rank.shape[1]
    experts = rank.shape[0]
    row = lax.broadcasted_iota(jnp.int32, (experts, cap, tok), 1).astype(F32)
    hit = rank[:, None, :] == row
    return jnp.where(hit, 1.0, 0.0).reshape(experts * cap, tok).astype(BF16)


def split3(x):
    hi = x.astype(BF16)
    rest = x - hi.astype(F32)
    mid = rest.astype(BF16)
    low = (rest - mid.astype(F32)).astype(BF16)
    return jnp.concatenate([hi, mid, low], axis=0)


def gather_kernel(u_ref, dy_ref, ids_ref, wr_ref, x_ref, d_ref, uall_ref, rank_ref, g_ref, prob_ref, gown_ref,
                  rcv, pbuf, xbuf, in_sem, send_sem, recv_sem, meta_send, meta_recv, out_sem, uout_sem):
    y, c, z = position()
    me = block_of(y, c, z)
    tok = u_ref.shape[0]
    d_model = u_ref.shape[1]
    experts = wr_ref.shape[0]
    local = rank_ref.shape[1]
    cap = pbuf.shape[0] // local
    blocks = rcv.shape[1]

    own_u = pltpu.make_async_copy(u_ref, rcv.at[0, me], in_sem.at[0])
    own_d = pltpu.make_async_copy(dy_ref, rcv.at[1, me], in_sem.at[1])
    own_u.start()
    own_d.start()

    def rdma(arr, s, kind, ep_to, z_to):
        return pltpu.make_async_remote_copy(
            src_ref=rcv.at[arr, s], dst_ref=rcv.at[arr, s], send_sem=send_sem.at[arr, s, kind],
            recv_sem=recv_sem.at[arr, s], device_id={"ep": ep_to, "etp": z_to}, device_id_type=MESH)

    ep_sib = y * 2 + 1 - c
    ep_y = (1 - y) * 2 + c
    ep_me = y * 2 + c

    def send_down(arr, s):
        return rdma(arr, s, 0, ep_me, jnp.maximum(z - 1, 0))

    def send_up(arr, s):
        return rdma(arr, s, 1, ep_me, jnp.minimum(z + 1, 3))

    def send_y(arr, s):
        return rdma(arr, s, 2, ep_y, z)

    def send_sib(arr, s):
        return rdma(arr, s, 3, ep_sib, z)

    for arr, own in ((0, own_u), (1, own_d)):
        own.wait()

        @pl.when(z > 0)
        def _():
            send_down(arr, me).start()

        @pl.when(z < 3)
        def _():
            send_up(arr, me).start()

        send_y(arr, me).start()
        send_sib(arr, me).start()

    logits = dot_nt(wr_ref[...], rcv[0, me])
    shifted = jnp.exp(logits - jnp.max(logits, axis=0, keepdims=True))
    prob = shifted / jnp.sum(shifted, axis=0, keepdims=True)
    expert_row = lax.broadcasted_iota(jnp.int32, (experts, tok), 0)
    chosen = expert_row == ids_ref[0:1, :]
    for j in range(1, ids_ref.shape[0]):
        chosen = chosen | (expert_row == ids_ref[j:j + 1, :])
    prob_ref[...] = jnp.zeros(prob_ref.shape, F32)
    prob_ref[:, 0:tok] = prob
    gown_ref[...] = jnp.full(gown_ref.shape, -1.0, F32)
    gown_ref[:, 0:tok] = jnp.where(chosen, prob, -1.0)
    g_ref[me] = gown_ref[pl.ds(pl.multiple_of(ep_me * local, local), local), :]

    def meta_copy(s):
        ep_to = s // 4
        return pltpu.make_async_remote_copy(
            src_ref=gown_ref.at[pl.ds(pl.multiple_of(ep_to * local, local), local), :], dst_ref=g_ref.at[me],
            send_sem=meta_send.at[s], recv_sem=meta_recv.at[me], device_id={"ep": ep_to, "etp": s % 4},
            device_id_type=MESH)

    def meta_wait(s):
        return pltpu.make_async_remote_copy(
            src_ref=gown_ref.at[pl.ds(0, local), :], dst_ref=g_ref.at[s], send_sem=meta_send.at[s],
            recv_sem=meta_recv.at[s], device_id={"ep": ep_me, "etp": z}, device_id_type=MESH)

    @pl.loop(1, blocks)
    def _(i):
        meta_copy((me + i) % blocks).start()

    lower = (lax.broadcasted_iota(jnp.int32, (LANES, LANES), 0) < lax.broadcasted_iota(jnp.int32, (LANES, LANES), 1))
    before = jnp.where(lower, 1.0, 0.0).astype(BF16)

    def out_copy(arr_is_dy, slot, s):
        return pltpu.make_async_copy(xbuf.at[slot], (d_ref if arr_is_dy else x_ref).at[s], out_sem.at[slot])

    def u_copy(s):
        return pltpu.make_async_copy(rcv.at[0, s], uall_ref.at[s], uout_sem.at[s])

    @pl.loop(0, 5)
    def _(t):
        for arr in (0, 1):
            @pl.when((t >= 1) & (t <= 3))
            def _():
                zb = near_order(z, t)
                s = block_of(y, c, zb)
                send_y(arr, s).wait_recv()

                @pl.when((zb < z) & (z < 3))
                def _():
                    send_up(arr, s).start()

                @pl.when((zb > z) & (z > 0))
                def _():
                    send_down(arr, s).start()

                send_y(arr, s).start()
                send_sib(arr, s).start()

        for arr in (0, 1):
            @pl.when(t >= 1)
            def _():
                s = block_of(1 - y, c, near_order(z, t - 1))
                send_y(arr, s).wait_recv()
                send_sib(arr, s).start()

        lo = 4 * (t // 4)
        hi = jnp.where(t == 0, 4, 8)

        @pl.loop(lo, hi)
        def _(i):
            typ = i // 4
            arr = (i // 2) % 2
            flip = i % 2
            core = c + flip - 2 * c * flip
            zb = near_order(z, t - typ)
            yb = y + typ - 2 * y * typ
            s = block_of(yb, core, zb)
            j = jnp.maximum(8 * t - 4, 0) + i - lo
            slot = j % 2

            @pl.when(flip == 1)
            def _():
                send_y(arr, s).wait_recv()

            @pl.when(arr == 0)
            def _():
                u_copy(s).start()

                @pl.when(s != me)
                def _():
                    meta_wait(s).wait_recv()

                mask = g_ref[s] >= 0.0
                rank = dot_nn(jnp.where(mask, 1.0, 0.0).astype(BF16), before)
                rank_ref[s] = jnp.where(mask, rank, -1.0)

            pbuf[...] = one_hot_slots(rank_ref[s][:, 0:tok], cap)

            @pl.when(j >= 2)
            def _():
                out_copy(False, slot, s).wait()

            @pl.loop(0, d_model // CHUNK)
            def _(n):
                cols = pl.ds(pl.multiple_of(n * CHUNK, CHUNK), CHUNK)
                xbuf[slot, :, cols] = dot_nn(pbuf[...], rcv[arr, s, :, cols]).astype(BF16)

            @pl.when(arr == 0)
            def _():
                out_copy(False, slot, s).start()

            @pl.when(arr == 1)
            def _():
                out_copy(True, slot, s).start()

    for slot in (0, 1):
        out_copy(False, slot, me).wait()

    @pl.loop(0, blocks)
    def _(s):
        u_copy(s).wait()

        @pl.when(s != me)
        def _():
            meta_copy(s).wait_send()

    @pl.loop(0, 4)
    def _(q):
        zb = near_order(z, q)
        s = block_of(y, c, zb)
        sy = block_of(1 - y, c, zb)
        for arr in (0, 1):
            @pl.when((z > 0) & (zb >= z))
            def _():
                send_down(arr, s).wait_send()

            @pl.when((z < 3) & (zb <= z))
            def _():
                send_up(arr, s).wait_send()

            send_y(arr, s).wait_send()
            send_sib(arr, s).wait_send()
            send_sib(arr, sy).wait_send()


def expert_kernel(te, tl, th, count, x_ref, d_ref, wg_ref, wu_ref, wd_ref, rank_ref, g_ref,
                  go_ref, dx_ref, dwg_ref, dwu_ref, dwd_ref, dg_ref):
    i = pl.program_id(0)

    @pl.when(i < count[0])
    def _():
        expert_tile(i, te, tl, th, x_ref, d_ref, wg_ref, wu_ref, wd_ref, rank_ref, g_ref, go_ref, dx_ref, dwg_ref, dwu_ref, dwd_ref, dg_ref)


def expert_tile(i, te, tl, th, x_ref, d_ref, wg_ref, wu_ref, wd_ref, rank_ref, g_ref,
                go_ref, dx_ref, dwg_ref, dwu_ref, dwd_ref, dg_ref):
    e = te[i]
    level = tl[i]
    half = th[i]
    rows = HALF * LEVEL_ROWS
    d_model = x_ref.shape[-1]
    fresh = (i == 0) | (te[jnp.maximum(i - 1, 0)] != e)

    x = x_ref[...].reshape(rows, d_model)
    dy = d_ref[...].reshape(rows, d_model)
    seg = pl.ds(pl.multiple_of(half * HALF, HALF), HALF)
    rank = rank_ref[e, seg, :]
    gate = g_ref[e, seg, :]
    slot = lax.broadcasted_iota(jnp.int32, (HALF, LEVEL_ROWS, LANES), 1) + level * LEVEL_ROWS
    hit = rank[:, None, :] == slot.astype(F32)
    g_slot = jnp.sum(jnp.where(hit, gate[:, None, :], 0.0), axis=2, keepdims=True).reshape(rows, 1)

    h1 = dot_nt(x, wg_ref[...]).astype(BF16).astype(F32)
    h3 = dot_nt(x, wu_ref[...]).astype(BF16).astype(F32)
    sig = jax.nn.sigmoid(h1)
    silu = h1 * sig
    act = (silu * h3).astype(BF16)
    out = dot_nn(act, wd_ref[...])
    dyf = dy.astype(F32)
    dg = jnp.sum(out * dyf, axis=1, keepdims=True)
    go_ref[...] = (out * g_slot).astype(BF16).reshape(go_ref.shape)
    do = (dyf * g_slot).astype(BF16)
    da = dot_nt(do, wd_ref[...]).astype(BF16).astype(F32)
    dh1 = (da * h3 * sig * (1.0 + h1 * (1.0 - sig))).astype(BF16)
    dh3 = (da * silu).astype(BF16)
    dx = dot_nn(dh1, wg_ref[...]) + dot_nn(dh3, wu_ref[...])
    dx_ref[...] = dx.astype(BF16).reshape(dx_ref.shape)
    dg_tok = jnp.sum(jnp.where(hit, dg.reshape(HALF, LEVEL_ROWS, 1), 0.0), axis=1)

    @pl.when(i == 0)
    def _():
        dg_ref[...] = jnp.zeros(dg_ref.shape, F32)

    dg_ref[e, seg, :] += dg_tok

    @pl.when(fresh)
    def _():
        dwd_ref[...] = dot_tn(act, do)
        dwg_ref[...] = dot_tn(dh1, x)
        dwu_ref[...] = dot_tn(dh3, x)

    @pl.when(jnp.logical_not(fresh))
    def _():
        dwd_ref[...] += dot_tn(act, do)
        dwg_ref[...] += dot_tn(dh1, x)
        dwu_ref[...] += dot_tn(dh3, x)


def scatter_kernel(go_ref, dx_ref, uall_ref, rank_ref, dgb_ref, prob_ref, gown_ref, u_ref, dy_ref, wr_ref,
                   yo_ref, du_ref, dwr_ref,
                   slots, pbuf, acc, sib_out, sib_in, y_out, y_in, z_out, z_in, dg_in, dl_all, ubuf,
                   ld_sem, sib_ss, sib_rs, y_ss, y_rs, z_ss, z_rs, dg_ss, dg_rs, dl_ss, dl_rs, u_sem):
    y, c, z = position()
    me = block_of(y, c, z)
    ep_me = y * 2 + c
    ep_sib = y * 2 + 1 - c
    ep_y = (1 - y) * 2 + c
    blocks, local, lanes = rank_ref.shape
    tok, d_model = u_ref.shape
    cap = pbuf.shape[0] // local
    experts = prob_ref.shape[0]

    def dg_copy(s, src):
        return pltpu.make_async_remote_copy(
            src_ref=dgb_ref.at[s], dst_ref=dg_in.at[src], send_sem=dg_ss.at[s], recv_sem=dg_rs.at[src],
            device_id={"ep": s // 4, "etp": s % 4}, device_id_type=MESH)

    def dl_copy(s, src):
        return pltpu.make_async_remote_copy(
            src_ref=dl_all.at[src], dst_ref=dl_all.at[src], send_sem=dl_ss.at[s], recv_sem=dl_rs.at[src],
            device_id={"ep": s // 4, "etp": s % 4}, device_id_type=MESH)

    def sib_copy(slot, arr, k):
        return pltpu.make_async_remote_copy(
            src_ref=sib_out.at[slot], dst_ref=sib_in.at[arr, k], send_sem=sib_ss.at[slot], recv_sem=sib_rs.at[arr, k],
            device_id={"ep": ep_sib, "etp": z}, device_id_type=MESH)

    def y_copy(arr, k):
        return pltpu.make_async_remote_copy(
            src_ref=y_out.at[arr, k], dst_ref=y_in.at[arr, k], send_sem=y_ss.at[arr, k], recv_sem=y_rs.at[arr, k],
            device_id={"ep": ep_y, "etp": z}, device_id_type=MESH)

    def z_copy(arr, k, slot, z_to):
        return pltpu.make_async_remote_copy(
            src_ref=z_out.at[arr, k], dst_ref=z_in.at[arr, slot], send_sem=z_ss.at[arr, k], recv_sem=z_rs.at[arr, slot],
            device_id={"ep": ep_me, "etp": z_to}, device_id_type=MESH)

    def plan(n):
        arr = jnp.where(n < 12, 0, jnp.where(n < 20, 1, jnp.where(n < 24, 0, 1)))
        phase = jnp.where(n < 8, 1, jnp.where(n < 12, 2, jnp.where(n < 20, 1, jnp.where(n < 24, 3, jnp.where(n < 28, 2, 3)))))
        off = jnp.where(n < 8, n, n % 4)
        off = jnp.where((n >= 12) & (n < 20), n - 12, off)
        k = jnp.where(phase == 1, off // 2, off)
        to_sib = jnp.where(phase == 1, 1 - off % 2, jnp.where(phase == 2, 1, 0))
        other = jnp.where(phase == 1, 1, 0)
        core = c + to_sib - 2 * c * to_sib
        col = y + other - 2 * y * other
        return arr, phase, k, to_sib, block_of(col, core, far_order(z, k))

    def start_load(n, slot):
        arr, phase, k, to_sib, s = plan(n)

        @pl.when(arr == 0)
        def _():
            pltpu.make_async_copy(go_ref.at[s], slots.at[slot], ld_sem.at[slot]).start()

        @pl.when(arr == 1)
        def _():
            pltpu.make_async_copy(dx_ref.at[s], slots.at[slot], ld_sem.at[slot]).start()

    start_load(0, 0)

    @pl.loop(1, blocks)
    def _(i):
        dg_copy((me + i) % blocks, me).start()

    dg_in[me] = dgb_ref[me]

    @pl.loop(0, 32)
    def _(n):
        slot = n % 2
        arr, phase, k, to_sib, s = plan(n)

        @pl.when(n < 31)
        def _():
            start_load(n + 1, 1 - slot)

        pbuf[...] = one_hot_slots(rank_ref[s][:, 0:tok], cap)
        pltpu.make_async_copy(go_ref.at[s], slots.at[slot], ld_sem.at[slot]).wait()

        @pl.loop(0, d_model // CHUNK)
        def _(m):
            cols = pl.ds(pl.multiple_of(m * CHUNK, CHUNK), CHUNK)
            acc[:, cols] = dot_tn(pbuf[...], slots[slot, :, cols])

        @pl.when(to_sib == 1)
        def _():
            idx = k + 4 * (phase - 1)
            out = idx % 2

            @pl.when((idx >= 2) | (arr == 1))
            def _():
                sib_copy(out, arr, idx).wait_send()

            sib_out[out] = acc[...].astype(BF16)
            sib_copy(out, arr, idx).start()

        @pl.when((phase == 1) & (to_sib == 0))
        def _():
            sib_copy(0, arr, k).wait_recv()
            y_out[arr, k] = (acc[...] + sib_in[arr, k].astype(F32)).astype(BF16)
            y_copy(arr, k).start()

        @pl.when(phase == 3)
        def _():
            sib_copy(0, arr, k + 4).wait_recv()
            y_copy(arr, k).wait_recv()
            acc[...] = acc[...] + sib_in[arr, k + 4].astype(F32) + y_in[arr, k].astype(F32)
            target = far_order(z, k)

            @pl.when(((target > z) & (z > 0)) | ((target < z) & (z < 3)) | ((target == z) & (z > 0)))
            def _():
                z_copy(arr, 0, target, z).wait_recv()
                acc[...] += z_in[arr, target].astype(F32)

            @pl.when((target == z) & (z < 3))
            def _():
                z_copy(arr, 0, 4, z).wait_recv()
                acc[...] += z_in[arr, 4].astype(F32)

            @pl.when(k < 3)
            def _():
                z_out[arr, k] = acc[...].astype(BF16)
                z_to = jnp.where(target > z, z + 1, z - 1)
                dst = jnp.where(target == z - 1, 4, target)
                z_copy(arr, k, dst, z_to).start()

            @pl.when((k == 3) & (arr == 0))
            def _():
                yo_ref[...] = (u_ref[...].astype(F32) + acc[...]).astype(BF16)

            @pl.when((k == 3) & (arr == 1))
            def _():
                dl3 = split3(dl_all[me][:, 0:tok])
                wr = wr_ref[...]
                router = dot_tn(dl3, jnp.concatenate([wr, wr, wr], axis=0))
                du_ref[...] = (dy_ref[...].astype(F32) + acc[...] + router).astype(BF16)

        @pl.when(n == 11)
        def _():
            @pl.loop(0, blocks)
            def _(b):
                @pl.when(b != me)
                def _():
                    dg_copy(me, b).wait_recv()

            d_gate = jnp.sum(dg_in[...].reshape(4, 4, local, lanes), axis=1).reshape(experts, lanes)
            d_prob = jnp.where(gown_ref[...] >= 0.0, d_gate, 0.0)
            prob = prob_ref[...]
            dl_all[me] = prob * (d_prob - jnp.sum(prob * d_prob, axis=0, keepdims=True))

            @pl.loop(1, blocks)
            def _(b):
                dl_copy((me + b) % blocks, me).start()

        @pl.when(n == 27)
        def _():
            dwr_ref[...] = jnp.zeros(dwr_ref.shape, F32)
            pltpu.make_async_copy(uall_ref.at[0], ubuf.at[0], u_sem.at[0]).start()

            @pl.loop(0, blocks)
            def _(b):
                us = b % 2

                @pl.when(b < blocks - 1)
                def _():
                    pltpu.make_async_copy(uall_ref.at[b + 1], ubuf.at[1 - us], u_sem.at[1 - us]).start()

                @pl.when(b != me)
                def _():
                    dl_copy(me, b).wait_recv()

                pltpu.make_async_copy(uall_ref.at[b], ubuf.at[us], u_sem.at[us]).wait()
                part = dot_nn(split3(dl_all[b][:, 0:tok]), ubuf[us])
                dwr_ref[...] += part[0:experts] + part[experts:2 * experts] + part[2 * experts:3 * experts]

    for out in (0, 1):
        sib_copy(out, 0, 0).wait_send()

    @pl.loop(0, 4)
    def _(k):
        for arr in (0, 1):
            y_copy(arr, k).wait_send()

            @pl.when(k < 3)
            def _():
                z_copy(arr, k, 0, z).wait_send()

    @pl.loop(0, blocks)
    def _(b):
        @pl.when(b != me)
        def _():
            dg_copy(b, me).wait_send()
            dl_copy(b, me).wait_send()


def work_list(rank, cap):
    local, blocks, lanes = rank.shape
    levels = cap // LEVEL_ROWS
    halves = blocks // HALF
    top = jnp.max(rank.reshape(local, halves, HALF * lanes), axis=2).astype(jnp.int32)
    level = jnp.arange(levels, dtype=jnp.int32)
    active = (level[None, :, None] * LEVEL_ROWS <= top[:, None, :]) | (level[None, :, None] == 0)
    flat = active.reshape(-1).astype(jnp.int32)
    total = flat.shape[0]
    idx = jnp.arange(total, dtype=jnp.int32)
    pos = jnp.sum(jnp.where(idx[None, :] < idx[:, None], flat[None, :], 0), axis=1)
    count = jnp.sum(flat)
    want = jnp.minimum(idx, count - 1)
    hit = (pos[None, :] == want[:, None]) & (flat[None, :] == 1)
    order = jnp.sum(jnp.where(hit, idx[None, :], 0), axis=1)
    return order // (levels * halves), (order // halves) % levels, order % halves, count.reshape(1)


def solution(mesh):
    ep_size = mesh.shape["ep"]
    etp_size = mesh.shape["etp"]
    blocks = ep_size * etp_size
    tok_spec = P(("dp", "ep", "etp"), None)
    col_spec = P("ep", None, "etp")
    row_spec = P("ep", "etp", None)
    in_specs = (tok_spec, tok_spec, tok_spec, P(None, None), col_spec, col_spec, row_spec)
    out_specs = (tok_spec, tok_spec, P(("dp", "ep"), None, "etp"), P(("dp", "ep"), None, "etp"), P(("dp", "ep"), "etp", None), P("dp", None))
    any_spec = pl.BlockSpec(memory_space=pl.ANY)
    vmem = pl.BlockSpec(memory_space=pltpu.VMEM)
    dma = pltpu.SemaphoreType.DMA

    def device_step(u_loc, dy_loc, ids_loc, w_router, w_gate, w_up, w_down):
        tok, d_model = u_loc.shape
        top_k = ids_loc.shape[1]
        experts = w_router.shape[1]
        local = w_gate.shape[0]
        ffn = w_gate.shape[2]
        cap = 96
        slots = local * cap
        ids_t = ids_loc.T
        wr_t = w_router.T
        wg_t = jnp.swapaxes(w_gate, 1, 2)
        wu_t = jnp.swapaxes(w_up, 1, 2)

        slot_shape = jax.ShapeDtypeStruct((blocks, slots, d_model), BF16)
        meta_shape = jax.ShapeDtypeStruct((blocks, local, LANES), F32)
        own_shape = jax.ShapeDtypeStruct((experts, LANES), F32)
        x_slots, d_slots, u_all, rank, gate, prob, g_own = pl.pallas_call(
            gather_kernel,
            name="gather",
            out_shape=(slot_shape, slot_shape, jax.ShapeDtypeStruct((blocks, tok, d_model), BF16), meta_shape, meta_shape, own_shape, own_shape),
            in_specs=[any_spec, any_spec, vmem, vmem],
            out_specs=(any_spec, any_spec, any_spec, vmem, vmem, vmem, vmem),
            scratch_shapes=[
                pltpu.VMEM((2, blocks, tok, d_model), BF16),
                pltpu.VMEM((slots, tok), BF16),
                pltpu.VMEM((2, slots, d_model), BF16),
                dma((2,)), dma((2, blocks, 4)), dma((2, blocks)), dma((blocks,)), dma((blocks,)), dma((2,)), dma((blocks,)),
            ],
            compiler_params=pltpu.CompilerParams(has_side_effects=True, vmem_limit_bytes=60 * 1024 * 1024),
        )(u_loc, dy_loc, ids_t, wr_t)

        rank_e = jnp.swapaxes(rank, 0, 1)
        gate_e = jnp.swapaxes(gate, 0, 1)
        te, tl, th, count = work_list(rank_e, cap)
        levels = cap // LEVEL_ROWS
        tiles = (blocks, local, levels, LEVEL_ROWS, d_model)

        def tile_map(i, te, tl, th, count):
            return th[i], te[i], tl[i], 0, 0

        def weight_map(i, te, tl, th, count):
            return te[i], 0, 0

        def whole(i, te, tl, th, count):
            return 0, 0, 0

        tile_spec = pl.BlockSpec((HALF, None, None, LEVEL_ROWS, d_model), tile_map)
        weight_spec = pl.BlockSpec((None, ffn, d_model), weight_map)
        meta_spec = pl.BlockSpec((local, blocks, LANES), whole)
        dw_shape = jax.ShapeDtypeStruct((local, ffn, d_model), F32)
        tile_shape = jax.ShapeDtypeStruct(tiles, BF16)
        go, dx, dwg, dwu, dwd, dg = pl.pallas_call(
            expert_kernel,
            name="experts",
            out_shape=(tile_shape, tile_shape, dw_shape, dw_shape, dw_shape, jax.ShapeDtypeStruct((local, blocks, LANES), F32)),
            grid_spec=pltpu.PrefetchScalarGridSpec(
                num_scalar_prefetch=4,
                grid=(local * levels * (blocks // HALF),),
                in_specs=[tile_spec, tile_spec, weight_spec, weight_spec, weight_spec, meta_spec, meta_spec],
                out_specs=[tile_spec, tile_spec, weight_spec, weight_spec, weight_spec, meta_spec],
            ),
            input_output_aliases={4: 0, 5: 1},
            compiler_params=pltpu.CompilerParams(vmem_limit_bytes=60 * 1024 * 1024, dimension_semantics=("arbitrary",)),
        )(te, tl, th, count, x_slots.reshape(tiles), d_slots.reshape(tiles), wg_t, wu_t, w_down, rank_e, gate_e)

        dg_blocks = jnp.swapaxes(dg, 0, 1)
        y_loc, du_loc, dwr_t = pl.pallas_call(
            scatter_kernel,
            name="scatter",
            out_shape=(jax.ShapeDtypeStruct((tok, d_model), BF16), jax.ShapeDtypeStruct((tok, d_model), BF16), jax.ShapeDtypeStruct((experts, d_model), F32)),
            in_specs=[any_spec, any_spec, any_spec] + [vmem] * 7,
            out_specs=(vmem, vmem, vmem),
            scratch_shapes=[
                pltpu.VMEM((2, slots, d_model), BF16),
                pltpu.VMEM((slots, tok), BF16),
                pltpu.VMEM((tok, d_model), F32),
                pltpu.VMEM((2, tok, d_model), BF16),
                pltpu.VMEM((2, 8, tok, d_model), BF16),
                pltpu.VMEM((2, 4, tok, d_model), BF16),
                pltpu.VMEM((2, 4, tok, d_model), BF16),
                pltpu.VMEM((2, 3, tok, d_model), BF16),
                pltpu.VMEM((2, 5, tok, d_model), BF16),
                pltpu.VMEM((blocks, local, LANES), F32),
                pltpu.VMEM((blocks, experts, LANES), F32),
                pltpu.VMEM((2, tok, d_model), BF16),
                dma((2,)), dma((2,)), dma((2, 8)), dma((2, 4)), dma((2, 4)), dma((2, 3)), dma((2, 5)),
                dma((blocks,)), dma((blocks,)), dma((blocks,)), dma((blocks,)), dma((2,)),
            ],
            compiler_params=pltpu.CompilerParams(has_side_effects=True, vmem_limit_bytes=60 * 1024 * 1024),
        )(go.reshape(slot_shape.shape), dx.reshape(slot_shape.shape), u_all, rank, dg_blocks, prob, g_own, u_loc, dy_loc, wr_t)

        dw_gate = jnp.swapaxes(dwg, 1, 2)
        dw_up = jnp.swapaxes(dwu, 1, 2)
        return y_loc, du_loc, dw_gate, dw_up, dwd, dwr_t.T

    return jax.shard_map(device_step, mesh=mesh, in_specs=in_specs, out_specs=out_specs, check_vma=False)
```

```python
import jax
import jax.numpy as jnp
from jax import lax
from jax.experimental import pallas as pl
from jax.experimental.pallas import tpu as pltpu
from jax.sharding import PartitionSpec as P

MESH = pl.DeviceIdType.MESH
F32 = jnp.float32
BF16 = jnp.bfloat16
LANES = 256
LEVEL_ROWS = 32
HALF = 8
CHUNK = 512


def dot_nn(a, b):
    return lax.dot_general(a, b, (((1,), (0,)), ((), ())), preferred_element_type=F32)


def dot_nt(a, b):
    return lax.dot_general(a, b, (((1,), (1,)), ((), ())), preferred_element_type=F32)


def dot_tn(a, b):
    return lax.dot_general(a, b, (((0,), (0,)), ((), ())), preferred_element_type=F32)


def position():
    ep = lax.axis_index("ep")
    z = lax.axis_index("etp")
    return ep // 2, ep % 2, z


def block_of(y, c, z):
    return (y * 2 + c) * 4 + z


def near_order(z, q):
    near = z - 1 + 2 * (1 - jnp.minimum(z, 1))
    far = 3 * (1 - z // 2)
    third = 6 - z - near - far
    return jnp.where(q == 0, z, jnp.where(q == 1, near, jnp.where(q == 2, third, far)))


def far_order(z, k):
    first = 3 * (1 - z // 2)
    second = (2 + 3 * z) % 5
    third = 1 + z % 2
    return jnp.where(k == 0, first, jnp.where(k == 1, second, jnp.where(k == 2, third, z)))


def one_hot_slots(rank, cap):
    tok = rank.shape[1]
    experts = rank.shape[0]
    row = lax.broadcasted_iota(jnp.int32, (experts, cap, tok), 1).astype(F32)
    hit = rank[:, None, :] == row
    return jnp.where(hit, 1.0, 0.0).reshape(experts * cap, tok).astype(BF16)


def one_hot_tokens(rank, cap):
    experts, tok = rank.shape
    lane = lax.broadcasted_iota(jnp.int32, (experts, experts * cap), 1)
    first = lax.broadcasted_iota(jnp.int32, (experts, experts * cap), 0) * cap
    mine = (lane >= first) & (lane < first + cap)
    spread = dot_tn(rank.astype(BF16), jnp.where(mine, 1.0, 0.0).astype(BF16))
    row = lax.broadcasted_iota(jnp.int32, (1, experts * cap), 1)
    for e in range(1, experts):
        row = row - jnp.where(lane[0:1] >= e * cap, cap, 0)
    return jnp.where(spread == row.astype(F32), 1.0, 0.0).astype(BF16)


def split3(x):
    hi = x.astype(BF16)
    rest = x - hi.astype(F32)
    mid = rest.astype(BF16)
    low = (rest - mid.astype(F32)).astype(BF16)
    return jnp.concatenate([hi, mid, low], axis=0)


def gather_kernel(u_ref, dy_ref, ids_ref, wr_ref, x_ref, d_ref, uall_ref, rank_ref, g_ref, prob_ref, gown_ref, cnt_ref,
                  rcv, pbuf, xbuf, in_sem, send_sem, recv_sem, meta_send, meta_recv, out_sem, uout_sem):
    y, c, z = position()
    me = block_of(y, c, z)
    tok = u_ref.shape[0]
    d_model = u_ref.shape[1]
    experts = wr_ref.shape[0]
    local = rank_ref.shape[1]
    cap = pbuf.shape[0] // local
    blocks = rcv.shape[1]

    own_u = pltpu.make_async_copy(u_ref, rcv.at[0, me], in_sem.at[0])
    own_d = pltpu.make_async_copy(dy_ref, rcv.at[1, me], in_sem.at[1])
    own_u.start()
    own_d.start()

    def rdma(arr, s, kind, ep_to, z_to):
        return pltpu.make_async_remote_copy(
            src_ref=rcv.at[arr, s], dst_ref=rcv.at[arr, s], send_sem=send_sem.at[arr, s, kind],
            recv_sem=recv_sem.at[arr, s], device_id={"ep": ep_to, "etp": z_to}, device_id_type=MESH)

    ep_sib = y * 2 + 1 - c
    ep_y = (1 - y) * 2 + c
    ep_me = y * 2 + c

    def send_down(arr, s):
        return rdma(arr, s, 0, ep_me, jnp.maximum(z - 1, 0))

    def send_up(arr, s):
        return rdma(arr, s, 1, ep_me, jnp.minimum(z + 1, 3))

    def send_y(arr, s):
        return rdma(arr, s, 2, ep_y, z)

    def send_sib(arr, s):
        return rdma(arr, s, 3, ep_sib, z)

    for arr, own in ((0, own_u), (1, own_d)):
        own.wait()

        @pl.when(z > 0)
        def _():
            send_down(arr, me).start()

        @pl.when(z < 3)
        def _():
            send_up(arr, me).start()

        send_y(arr, me).start()
        send_sib(arr, me).start()

    logits = dot_nt(wr_ref[...], rcv[0, me])
    shifted = jnp.exp(logits - jnp.max(logits, axis=0, keepdims=True))
    prob = shifted / jnp.sum(shifted, axis=0, keepdims=True)
    expert_row = lax.broadcasted_iota(jnp.int32, (experts, tok), 0)
    chosen = expert_row == ids_ref[0:1, :]
    for j in range(1, ids_ref.shape[0]):
        chosen = chosen | (expert_row == ids_ref[j:j + 1, :])
    prob_ref[...] = jnp.zeros(prob_ref.shape, F32)
    prob_ref[:, 0:tok] = prob
    gown_ref[...] = jnp.full(gown_ref.shape, -1.0, F32)
    gown_ref[:, 0:tok] = jnp.where(chosen, prob, -1.0)
    g_ref[me] = gown_ref[pl.ds(pl.multiple_of(ep_me * local, local), local), :]

    def meta_copy(s):
        ep_to = s // 4
        return pltpu.make_async_remote_copy(
            src_ref=gown_ref.at[pl.ds(pl.multiple_of(ep_to * local, local), local), :], dst_ref=g_ref.at[me],
            send_sem=meta_send.at[s], recv_sem=meta_recv.at[me], device_id={"ep": ep_to, "etp": s % 4},
            device_id_type=MESH)

    def meta_wait(s):
        return pltpu.make_async_remote_copy(
            src_ref=gown_ref.at[pl.ds(0, local), :], dst_ref=g_ref.at[s], send_sem=meta_send.at[s],
            recv_sem=meta_recv.at[s], device_id={"ep": ep_me, "etp": z}, device_id_type=MESH)

    @pl.loop(1, blocks)
    def _(i):
        meta_copy((me + i) % blocks).start()

    lower = (lax.broadcasted_iota(jnp.int32, (LANES, LANES), 0) < lax.broadcasted_iota(jnp.int32, (LANES, LANES), 1))
    before = jnp.where(lower, 1.0, 0.0).astype(BF16)

    def out_copy(arr_is_dy, slot, s):
        return pltpu.make_async_copy(xbuf.at[slot], (d_ref if arr_is_dy else x_ref).at[s], out_sem.at[slot])

    def u_copy(s):
        return pltpu.make_async_copy(rcv.at[0, s], uall_ref.at[s], uout_sem.at[s])

    @pl.loop(0, 5)
    def _(t):
        for arr in (0, 1):
            @pl.when((t >= 1) & (t <= 3))
            def _():
                zb = near_order(z, t)
                s = block_of(y, c, zb)
                send_y(arr, s).wait_recv()

                @pl.when((zb < z) & (z < 3))
                def _():
                    send_up(arr, s).start()

                @pl.when((zb > z) & (z > 0))
                def _():
                    send_down(arr, s).start()

                send_y(arr, s).start()
                send_sib(arr, s).start()

        for arr in (0, 1):
            @pl.when(t >= 1)
            def _():
                s = block_of(1 - y, c, near_order(z, t - 1))
                send_y(arr, s).wait_recv()
                send_sib(arr, s).start()

        lo = 4 * (t // 4)
        hi = jnp.where(t == 0, 4, 8)

        @pl.loop(lo, hi)
        def _(i):
            typ = i // 4
            arr = (i // 2) % 2
            flip = i % 2
            core = c + flip - 2 * c * flip
            zb = near_order(z, t - typ)
            yb = y + typ - 2 * y * typ
            s = block_of(yb, core, zb)
            j = jnp.maximum(8 * t - 4, 0) + i - lo
            slot = j % 2

            @pl.when(flip == 1)
            def _():
                send_y(arr, s).wait_recv()

            @pl.when(arr == 0)
            def _():
                u_copy(s).start()

                @pl.when(s != me)
                def _():
                    meta_wait(s).wait_recv()

                mask = g_ref[s] >= 0.0
                ones = jnp.where(mask, 1.0, 0.0)
                rank = dot_nn(ones.astype(BF16), before)
                cnt_ref[s] = jnp.broadcast_to(jnp.sum(ones, axis=1, keepdims=True), cnt_ref.shape[1:]).astype(jnp.int32)
                rank_ref[s] = jnp.where(mask, rank, -1.0)

            pbuf[...] = one_hot_slots(rank_ref[s][:, 0:tok], cap)

            @pl.when(j >= 2)
            def _():
                out_copy(False, slot, s).wait()

            @pl.loop(0, d_model // CHUNK)
            def _(n):
                cols = pl.ds(pl.multiple_of(n * CHUNK, CHUNK), CHUNK)
                xbuf[slot, :, :, :, cols] = dot_nn(pbuf[...], rcv[arr, s, :, cols]).astype(BF16).reshape(xbuf.shape[1:4] + (CHUNK,))

            @pl.when(arr == 0)
            def _():
                out_copy(False, slot, s).start()

            @pl.when(arr == 1)
            def _():
                out_copy(True, slot, s).start()

    for slot in (0, 1):
        out_copy(False, slot, me).wait()

    @pl.loop(0, blocks)
    def _(s):
        u_copy(s).wait()

        @pl.when(s != me)
        def _():
            meta_copy(s).wait_send()

    @pl.loop(0, 4)
    def _(q):
        zb = near_order(z, q)
        s = block_of(y, c, zb)
        sy = block_of(1 - y, c, zb)
        for arr in (0, 1):
            @pl.when((z > 0) & (zb >= z))
            def _():
                send_down(arr, s).wait_send()

            @pl.when((z < 3) & (zb <= z))
            def _():
                send_up(arr, s).wait_send()

            send_y(arr, s).wait_send()
            send_sib(arr, s).wait_send()
            send_sib(arr, sy).wait_send()


class ExpertTiles:
    def __init__(self, x_in, d_in, go, dx, wg, wu, wd, te, tk, tn, sg, xb, db, gob, dxb, wb, in_sem, out_sem, w_sem):
        self.te, self.tk, self.tn, self.sg = te, tk, tn, sg
        self.x_in, self.d_in, self.go, self.dx = x_in, d_in, go, dx
        self.w = (wg, wu, wd)
        self.xb, self.db, self.gob, self.dxb, self.wb = xb, db, gob, dxb, wb
        self.in_sem, self.out_sem, self.w_sem = in_sem, out_sem, w_sem

    def seg(self, ref, i, j):
        at = self.sg[i * HALF + j]
        return ref.at[at // 4, self.te[i], at % 4]

    def half(self, ref, i):
        return ref.at[pl.ds(pl.multiple_of(self.tk[i] * HALF, HALF), HALF), self.te[i], 0]

    def each(self, i, slot, act, moves, sem):
        @pl.when(self.tk[i] < 2)
        def _():
            for a, (hbm, buf, out) in enumerate(moves):
                ends = (buf.at[slot], self.half(hbm, i)) if out else (self.half(hbm, i), buf.at[slot])
                act(pltpu.make_async_copy(*ends, sem.at[a, slot, HALF]))

        for j in range(HALF):
            @pl.when((self.tk[i] == 2) & (j < self.tn[i]))
            def _():
                for a, (hbm, buf, out) in enumerate(moves):
                    ends = (buf.at[slot, j], self.seg(hbm, i, j)) if out else (self.seg(hbm, i, j), buf.at[slot, j])
                    act(pltpu.make_async_copy(*ends, sem.at[a, slot, j]))

    def load(self, i, slot, act):
        self.each(i, slot, act, ((self.x_in, self.xb, False), (self.d_in, self.db, False)), self.in_sem)

    def store(self, i, slot, act):
        self.each(i, slot, act, ((self.go, self.gob, True), (self.dx, self.dxb, True)), self.out_sem)

    def weights(self, e, p):
        return [pltpu.make_async_copy(src.at[e], self.wb.at[p, j], self.w_sem.at[p, j]) for j, src in enumerate(self.w)]

    def run(self, i, slot, p, fresh, dwb, dob, sgb, rank_ref, g_ref, dg_ref):
        rows = HALF * LEVEL_ROWS
        d_model = self.xb.shape[-1]
        one = pl.ds(self.te[i], 1)
        for j in range(HALF):
            at = self.sg[i * HALF + j]
            level = jnp.where(j < self.tn[i], at % 4, 8) * LEVEL_ROWS
            sgb[0, pl.ds(j, 1), :] = rank_ref[at // 4, one, :] - level.astype(F32)
            sgb[1, pl.ds(j, 1), :] = g_ref[at // 4, one, :]
        row = lax.broadcasted_iota(jnp.int32, (HALF, LEVEL_ROWS, LANES), 1)
        hit = sgb[0][:, None, :] == row.astype(F32)
        g_slot = jnp.sum(jnp.where(hit, sgb[1][:, None, :], 0.0), axis=2, keepdims=True).reshape(rows, 1)
        x = self.xb[slot].reshape(rows, d_model)
        h1 = dot_nt(x, self.wb[p, 0]).astype(BF16).astype(F32)
        h3 = dot_nt(x, self.wb[p, 1]).astype(BF16).astype(F32)
        sig = jax.nn.sigmoid(h1)
        silu = h1 * sig
        act = (silu * h3).astype(BF16)
        chunks = [slice(n, n + CHUNK) for n in range(0, d_model, CHUNK)]
        dg = jnp.zeros((rows, 1), F32)
        da = jnp.zeros((rows, act.shape[1]), F32)
        for cols in chunks:
            out = dot_nn(act, self.wb[p, 2, :, cols])
            dy = self.db[slot, :, :, cols].reshape(rows, CHUNK).astype(F32)
            dg = dg + jnp.sum(out * dy, axis=1, keepdims=True)
            self.gob[slot, :, :, cols] = (out * g_slot).astype(BF16).reshape(HALF, LEVEL_ROWS, CHUNK)
            do = (dy * g_slot).astype(BF16)
            dob[:, cols] = do
            da = da + dot_nt(do, self.wb[p, 2, :, cols])
        da = da.astype(BF16).astype(F32)
        dh1 = (da * h3 * sig * (1.0 + h1 * (1.0 - sig))).astype(BF16)
        dh3 = (da * silu).astype(BF16)
        for cols in chunks:
            dx = dot_nn(dh1, self.wb[p, 0, :, cols]) + dot_nn(dh3, self.wb[p, 1, :, cols])
            self.dxb[slot, :, :, cols] = dx.astype(BF16).reshape(HALF, LEVEL_ROWS, CHUNK)
        sgb[0] = jnp.sum(jnp.where(hit, dg.reshape(HALF, LEVEL_ROWS, 1), 0.0), axis=1)
        for j in range(HALF):
            dg_ref[self.sg[i * HALF + j] // 4, one, :] += sgb[0, pl.ds(j, 1), :]

        def add_dw(first):
            for cols in chunks:
                xc = self.xb[slot, :, :, cols].reshape(rows, CHUNK)
                for j, (left, right) in enumerate(((dh1, xc), (dh3, xc), (act, dob[:, cols]))):
                    part = dot_tn(left, right)
                    dwb[p, j, :, cols] = part if first else dwb[p, j, :, cols] + part

        @pl.when(fresh)
        def _():
            add_dw(True)

        @pl.when(jnp.logical_not(fresh))
        def _():
            add_dw(False)


def expert_kernel(cnt, x_hbm, d_hbm, wg_hbm, wu_hbm, wd_hbm, rank_ref, g_ref, go_hbm, dx_hbm, dwg_hbm, dwu_hbm, dwd_hbm, dg_ref,
                  te, tk, tn, sg, xb, db, gob, dxb, wb, dwb, dob, sgb, in_sem, out_sem, w_sem, dw_sem):
    local = wg_hbm.shape[0]
    levels = x_hbm.shape[2]
    blocks = x_hbm.shape[0]
    halves = blocks // HALF
    tiles = ExpertTiles(x_hbm, d_hbm, go_hbm, dx_hbm, wg_hbm, wu_hbm, wd_hbm, te, tk, tn, sg, xb, db, gob, dxb, wb, in_sem, out_sem, w_sem)

    def start(copy):
        copy.start()

    def wait(copy):
        copy.wait()

    def dw_out(e, p):
        return [pltpu.make_async_copy(dwb.at[p, j], dst.at[e], dw_sem.at[p, j]) for j, dst in enumerate((dwg_hbm, dwu_hbm, dwd_hbm))]

    te[0] = 0
    tk[0] = 0
    tn[0] = HALF
    for copy in tiles.weights(0, 0):
        copy.start()
    tiles.load(0, 0, start)
    dg_ref[...] = jnp.zeros(dg_ref.shape, F32)

    def add_expert(e, n):
        for h in range(halves):
            te[n + h] = e
            tk[n + h] = h
            tn[n + h] = HALF
            for j in range(HALF):
                sg[(n + h) * HALF + j] = (h * HALF + j) * 4
        n = n + halves

        def add_block(b, m):
            held = cnt[b, e]
            for level in range(1, levels):
                sg[n * HALF + m] = b * 4 + level
                m = m + jnp.where(held > level * LEVEL_ROWS, 1, 0)
            return m

        m = lax.fori_loop(0, blocks, add_block, 0)
        for j in range(HALF):
            sg[n * HALF + m + j] = 0
        extra = (m + HALF - 1) // HALF

        def add_tile(k, carry):
            te[n + k] = e
            tk[n + k] = 2
            tn[n + k] = jnp.minimum(m - k * HALF, HALF)
            return carry

        lax.fori_loop(0, extra, add_tile, 0)
        return n + extra

    count = lax.fori_loop(0, local, add_expert, 0)
    te[count] = local

    def step(i, carry):
        slot = i % 2
        e = te[i]
        p = e % 2
        fresh = (i == 0) | (te[jnp.maximum(i - 1, 0)] != e)
        last = te[i + 1] != e

        @pl.when(i + 1 < count)
        def _():
            tiles.load(i + 1, 1 - slot, start)

        @pl.when(fresh)
        def _():
            @pl.when(e + 1 < local)
            def _():
                for copy in tiles.weights(e + 1, 1 - p):
                    copy.start()

            for copy in tiles.weights(e, p):
                copy.wait()

            @pl.when(e >= 2)
            def _():
                for copy in dw_out(e, p):
                    copy.wait()

        tiles.load(i, slot, wait)

        @pl.when(i >= 2)
        def _():
            tiles.store(i - 2, slot, wait)

        tiles.run(i, slot, p, fresh, dwb, dob, sgb, rank_ref, g_ref, dg_ref)
        tiles.store(i, slot, start)

        @pl.when(last)
        def _():
            for copy in dw_out(e, p):
                copy.start()

        return carry

    lax.fori_loop(0, count, step, 0)
    for p in (0, 1):
        i = count - 2 + p
        tiles.store(i, i % 2, wait)
        for copy in dw_out(0, p):
            copy.wait()


def scatter_kernel(go_ref, dx_ref, uall_ref, rank_ref, dgb_ref, prob_ref, gown_ref, u_ref, dy_ref, wr_ref,
                   yo_ref, du_ref, dwr_ref,
                   slots, pbuf, acc, sib_out, sib_in, y_out, y_in, z_out, z_in, dg_in, dl_all, ubuf,
                   ld_sem, sib_ss, sib_rs, y_ss, y_rs, z_ss, z_rs, dg_ss, dg_rs, dl_ss, dl_rs, u_sem):
    y, c, z = position()
    me = block_of(y, c, z)
    ep_me = y * 2 + c
    ep_sib = y * 2 + 1 - c
    ep_y = (1 - y) * 2 + c
    blocks, local, lanes = rank_ref.shape
    tok, d_model = u_ref.shape
    cap = pbuf.shape[1] // local
    experts = prob_ref.shape[0]

    def dg_copy(s, src):
        return pltpu.make_async_remote_copy(
            src_ref=dgb_ref.at[s], dst_ref=dg_in.at[src], send_sem=dg_ss.at[s], recv_sem=dg_rs.at[src],
            device_id={"ep": s // 4, "etp": s % 4}, device_id_type=MESH)

    def dl_copy(s, src):
        return pltpu.make_async_remote_copy(
            src_ref=dl_all.at[src], dst_ref=dl_all.at[src], send_sem=dl_ss.at[s], recv_sem=dl_rs.at[src],
            device_id={"ep": s // 4, "etp": s % 4}, device_id_type=MESH)

    def sib_copy(slot, arr, k):
        return pltpu.make_async_remote_copy(
            src_ref=sib_out.at[slot], dst_ref=sib_in.at[arr, k], send_sem=sib_ss.at[slot], recv_sem=sib_rs.at[arr, k],
            device_id={"ep": ep_sib, "etp": z}, device_id_type=MESH)

    def y_copy(arr, k):
        return pltpu.make_async_remote_copy(
            src_ref=y_out.at[arr, k], dst_ref=y_in.at[arr, k], send_sem=y_ss.at[arr, k], recv_sem=y_rs.at[arr, k],
            device_id={"ep": ep_y, "etp": z}, device_id_type=MESH)

    def z_copy(arr, k, slot, z_to):
        return pltpu.make_async_remote_copy(
            src_ref=z_out.at[arr, k], dst_ref=z_in.at[arr, slot], send_sem=z_ss.at[arr, k], recv_sem=z_rs.at[arr, slot],
            device_id={"ep": ep_me, "etp": z_to}, device_id_type=MESH)

    def plan(n):
        arr = jnp.where(n < 12, 0, jnp.where(n < 20, 1, jnp.where(n < 24, 0, 1)))
        phase = jnp.where(n < 8, 1, jnp.where(n < 12, 2, jnp.where(n < 20, 1, jnp.where(n < 24, 3, jnp.where(n < 28, 2, 3)))))
        off = jnp.where(n < 8, n, n % 4)
        off = jnp.where((n >= 12) & (n < 20), n - 12, off)
        k = jnp.where(phase == 1, off // 2, off)
        to_sib = jnp.where(phase == 1, 1 - off % 2, jnp.where(phase == 2, 1, 0))
        other = jnp.where(phase == 1, 1, 0)
        core = c + to_sib - 2 * c * to_sib
        col = y + other - 2 * y * other
        return arr, phase, k, to_sib, block_of(col, core, far_order(z, k))

    def start_load(n, slot):
        arr, phase, k, to_sib, s = plan(n)

        @pl.when(arr == 0)
        def _():
            pltpu.make_async_copy(go_ref.at[s], slots.at[slot], ld_sem.at[slot]).start()

        @pl.when(arr == 1)
        def _():
            pltpu.make_async_copy(dx_ref.at[s], slots.at[slot], ld_sem.at[slot]).start()

    start_load(0, 0)

    @pl.loop(1, blocks)
    def _(i):
        dg_copy((me + i) % blocks, me).start()

    dg_in[me] = dgb_ref[me]
    dwr_ref[...] = jnp.zeros(dwr_ref.shape, F32)

    def u_load(b):
        return pltpu.make_async_copy(uall_ref.at[b], ubuf.at[b % 2], u_sem.at[b % 2])

    @pl.loop(0, 32)
    def _(n):
        slot = n % 2
        arr, phase, k, to_sib, s = plan(n)

        @pl.when(n < 31)
        def _():
            start_load(n + 1, 1 - slot)

        pbuf[...] = one_hot_tokens(rank_ref[s][:, 0:tok], cap)
        pltpu.make_async_copy(go_ref.at[s], slots.at[slot], ld_sem.at[slot]).wait()

        @pl.loop(0, d_model // CHUNK)
        def _(m):
            cols = pl.ds(pl.multiple_of(m * CHUNK, CHUNK), CHUNK)
            acc[:, cols] = dot_nn(pbuf[...], slots[slot, :, cols])

        @pl.when(n == 1)
        def _():
            @pl.loop(0, blocks)
            def _(b):
                @pl.when(b != me)
                def _():
                    dg_copy(me, b).wait_recv()

            d_gate = jnp.sum(dg_in[...].reshape(4, 4, local, lanes), axis=1).reshape(experts, lanes)
            d_prob = jnp.where(gown_ref[...] >= 0.0, d_gate, 0.0)
            prob = prob_ref[...]
            dl_all[me] = prob * (d_prob - jnp.sum(prob * d_prob, axis=0, keepdims=True))

            @pl.loop(1, blocks)
            def _(b):
                dl_copy((me + b) % blocks, me).start()

        @pl.when(to_sib == 1)
        def _():
            idx = k + 4 * (phase - 1)
            out = idx % 2

            @pl.when((idx >= 2) | (arr == 1))
            def _():
                sib_copy(out, arr, idx).wait_send()

            sib_out[out] = acc[...].astype(BF16)
            sib_copy(out, arr, idx).start()

        @pl.when((phase == 1) & (to_sib == 0))
        def _():
            sib_copy(0, arr, k).wait_recv()
            y_out[arr, k] = (acc[...] + sib_in[arr, k].astype(F32)).astype(BF16)
            y_copy(arr, k).start()

        @pl.when(phase == 3)
        def _():
            sib_copy(0, arr, k + 4).wait_recv()
            y_copy(arr, k).wait_recv()
            acc[...] = acc[...] + sib_in[arr, k + 4].astype(F32) + y_in[arr, k].astype(F32)
            target = far_order(z, k)

            @pl.when(((target > z) & (z > 0)) | ((target < z) & (z < 3)) | ((target == z) & (z > 0)))
            def _():
                z_copy(arr, 0, target, z).wait_recv()
                acc[...] += z_in[arr, target].astype(F32)

            @pl.when((target == z) & (z < 3))
            def _():
                z_copy(arr, 0, 4, z).wait_recv()
                acc[...] += z_in[arr, 4].astype(F32)

            @pl.when(k < 3)
            def _():
                z_out[arr, k] = acc[...].astype(BF16)
                z_to = jnp.where(target > z, z + 1, z - 1)
                dst = jnp.where(target == z - 1, 4, target)
                z_copy(arr, k, dst, z_to).start()

            @pl.when((k == 3) & (arr == 0))
            def _():
                yo_ref[...] = (u_ref[...].astype(F32) + acc[...]).astype(BF16)

            @pl.when((k == 3) & (arr == 1))
            def _():
                dl3 = split3(dl_all[me][:, 0:tok])
                wr = wr_ref[...]
                router = dot_tn(dl3, jnp.concatenate([wr, wr, wr], axis=0))
                du_ref[...] = (dy_ref[...].astype(F32) + acc[...] + router).astype(BF16)

        @pl.when((n >= 11) & (n < 27))
        def _():
            u_load(n - 11).start()

        @pl.when((n >= 12) & (n < 28))
        def _():
            b = n - 12

            @pl.when(b != me)
            def _():
                dl_copy(me, b).wait_recv()

            u_load(b).wait()
            part = dot_nn(split3(dl_all[b][:, 0:tok]), ubuf[b % 2])
            dwr_ref[...] += part[0:experts] + part[experts:2 * experts] + part[2 * experts:3 * experts]

    for out in (0, 1):
        sib_copy(out, 0, 0).wait_send()

    @pl.loop(0, 4)
    def _(k):
        for arr in (0, 1):
            y_copy(arr, k).wait_send()

            @pl.when(k < 3)
            def _():
                z_copy(arr, k, 0, z).wait_send()

    @pl.loop(0, blocks)
    def _(b):
        @pl.when(b != me)
        def _():
            dg_copy(b, me).wait_send()
            dl_copy(b, me).wait_send()


def solution(mesh):
    ep_size = mesh.shape["ep"]
    etp_size = mesh.shape["etp"]
    blocks = ep_size * etp_size
    tok_spec = P(("dp", "ep", "etp"), None)
    col_spec = P("ep", None, "etp")
    row_spec = P("ep", "etp", None)
    in_specs = (tok_spec, tok_spec, tok_spec, P(None, None), col_spec, col_spec, row_spec)
    out_specs = (tok_spec, tok_spec, P(("dp", "ep"), None, "etp"), P(("dp", "ep"), None, "etp"), P(("dp", "ep"), "etp", None), P("dp", None))
    any_spec = pl.BlockSpec(memory_space=pl.ANY)
    vmem = pl.BlockSpec(memory_space=pltpu.VMEM)
    dma = pltpu.SemaphoreType.DMA

    def device_step(u_loc, dy_loc, ids_loc, w_router, w_gate, w_up, w_down):
        tok, d_model = u_loc.shape
        top_k = ids_loc.shape[1]
        experts = w_router.shape[1]
        local = w_gate.shape[0]
        ffn = w_gate.shape[2]
        cap = 96
        slots = local * cap
        ids_t = ids_loc.T
        wr_t = w_router.T
        wg_t = jnp.swapaxes(w_gate, 1, 2)
        wu_t = jnp.swapaxes(w_up, 1, 2)

        levels = cap // LEVEL_ROWS
        tile_shape = jax.ShapeDtypeStruct((blocks, local, levels, LEVEL_ROWS, d_model), BF16)
        dw_shape = jax.ShapeDtypeStruct((local, ffn, d_model), F32)
        meta_shape = jax.ShapeDtypeStruct((blocks, local, LANES), F32)
        own_shape = jax.ShapeDtypeStruct((experts, LANES), F32)
        tile_buf = pltpu.VMEM((2, HALF, LEVEL_ROWS, d_model), BF16)
        weight_buf = pltpu.VMEM((2, 3, ffn, d_model), BF16)
        x_slots, d_slots, u_all, rank, gate, prob, g_own, counts = pl.pallas_call(
            gather_kernel,
            name="gather",
            out_shape=(tile_shape, tile_shape, jax.ShapeDtypeStruct((blocks, tok, d_model), BF16), meta_shape, meta_shape, own_shape, own_shape,
                       jax.ShapeDtypeStruct((blocks, local, 128), jnp.int32)),
            in_specs=[any_spec, any_spec, vmem, vmem],
            out_specs=(any_spec, any_spec, any_spec, vmem, vmem, vmem, vmem, vmem),
            scratch_shapes=[
                pltpu.VMEM((2, blocks, tok, d_model), BF16),
                pltpu.VMEM((slots, tok), BF16),
                pltpu.VMEM((2, local, levels, LEVEL_ROWS, d_model), BF16),
                dma((2,)), dma((2, blocks, 4)), dma((2, blocks)), dma((blocks,)), dma((blocks,)), dma((2,)), dma((blocks,)),
            ],
            compiler_params=pltpu.CompilerParams(has_side_effects=True, vmem_limit_bytes=60 * 1024 * 1024),
        )(u_loc, dy_loc, ids_t, wr_t)

        max_tiles = local * levels * (blocks // HALF) + 8
        smem_list = pltpu.SMEM((max_tiles,), jnp.int32)
        smem = pl.BlockSpec(memory_space=pltpu.SMEM)
        go, dx, dwg, dwu, dwd, dg_blocks = pl.pallas_call(
            expert_kernel,
            name="experts",
            out_shape=(tile_shape, tile_shape, dw_shape, dw_shape, dw_shape, meta_shape),
            in_specs=[smem] + [any_spec] * 5 + [vmem] * 2,
            out_specs=(any_spec,) * 5 + (vmem,),
            scratch_shapes=[
                smem_list, smem_list, smem_list, pltpu.SMEM((max_tiles * HALF,), jnp.int32), tile_buf, tile_buf, tile_buf, tile_buf, weight_buf,
                pltpu.VMEM((2, 3, ffn, d_model), F32),
                pltpu.VMEM((HALF * LEVEL_ROWS, d_model), BF16),
                pltpu.VMEM((2, HALF, LANES), F32),
                dma((2, 2, HALF + 1)), dma((2, 2, HALF + 1)), dma((2, 3)), dma((2, 3)),
            ],
            input_output_aliases={1: 0, 2: 1},
            compiler_params=pltpu.CompilerParams(vmem_limit_bytes=60 * 1024 * 1024),
        )(counts[:, :, 0], x_slots, d_slots, wg_t, wu_t, w_down, rank, gate)

        slot_shape = (blocks, slots, d_model)
        y_loc, du_loc, dwr_t = pl.pallas_call(
            scatter_kernel,
            name="scatter",
            out_shape=(jax.ShapeDtypeStruct((tok, d_model), BF16), jax.ShapeDtypeStruct((tok, d_model), BF16), jax.ShapeDtypeStruct((experts, d_model), F32)),
            in_specs=[any_spec, any_spec, any_spec] + [vmem] * 7,
            out_specs=(vmem, vmem, vmem),
            scratch_shapes=[
                pltpu.VMEM((2, slots, d_model), BF16),
                pltpu.VMEM((tok, slots), BF16),
                pltpu.VMEM((tok, d_model), F32),
                pltpu.VMEM((2, tok, d_model), BF16),
                pltpu.VMEM((2, 8, tok, d_model), BF16),
                pltpu.VMEM((2, 4, tok, d_model), BF16),
                pltpu.VMEM((2, 4, tok, d_model), BF16),
                pltpu.VMEM((2, 3, tok, d_model), BF16),
                pltpu.VMEM((2, 5, tok, d_model), BF16),
                pltpu.VMEM((blocks, local, LANES), F32),
                pltpu.VMEM((blocks, experts, LANES), F32),
                pltpu.VMEM((2, tok, d_model), BF16),
                dma((2,)), dma((2,)), dma((2, 8)), dma((2, 4)), dma((2, 4)), dma((2, 3)), dma((2, 5)),
                dma((blocks,)), dma((blocks,)), dma((blocks,)), dma((blocks,)), dma((2,)),
            ],
            compiler_params=pltpu.CompilerParams(has_side_effects=True, vmem_limit_bytes=60 * 1024 * 1024),
        )(go.reshape(slot_shape), dx.reshape(slot_shape), u_all, rank, dg_blocks, prob, g_own, u_loc, dy_loc, wr_t)

        dw_gate = jnp.swapaxes(dwg, 1, 2)
        dw_up = jnp.swapaxes(dwu, 1, 2)
        return y_loc, du_loc, dw_gate, dw_up, dwd, dwr_t.T

    return jax.shard_map(device_step, mesh=mesh, in_specs=in_specs, out_specs=out_specs, check_vma=False)
```

```python
import jax
import jax.numpy as jnp
from jax import lax
from jax.experimental import pallas as pl
from jax.experimental.pallas import tpu as pltpu
from jax.sharding import PartitionSpec as P

MESH = pl.DeviceIdType.MESH
F32 = jnp.float32
BF16 = jnp.bfloat16
LANES = 256
LEVEL_ROWS = 32
HALF = 8
CHUNK = 512
TAIL = 16


def dot_nn(a, b):
    return lax.dot_general(a, b, (((1,), (0,)), ((), ())), preferred_element_type=F32)


def dot_nt(a, b):
    return lax.dot_general(a, b, (((1,), (1,)), ((), ())), preferred_element_type=F32)


def dot_tn(a, b):
    return lax.dot_general(a, b, (((0,), (0,)), ((), ())), preferred_element_type=F32)


def position():
    ep = lax.axis_index("ep")
    z = lax.axis_index("etp")
    return ep // 2, ep % 2, z


def block_of(y, c, z):
    return (y * 2 + c) * 4 + z


def near_order(z, q):
    near = z - 1 + 2 * (1 - jnp.minimum(z, 1))
    far = 3 * (1 - z // 2)
    third = 6 - z - near - far
    return jnp.where(q == 0, z, jnp.where(q == 1, near, jnp.where(q == 2, third, far)))


def far_order(z, k):
    first = 3 * (1 - z // 2)
    second = (2 + 3 * z) % 5
    third = 1 + z % 2
    return jnp.where(k == 0, first, jnp.where(k == 1, second, jnp.where(k == 2, third, z)))


def one_hot_slots(rank, cap):
    tok = rank.shape[1]
    experts = rank.shape[0]
    row = lax.broadcasted_iota(jnp.int32, (experts, cap, tok), 1).astype(F32)
    hit = rank[:, None, :] == row
    return jnp.where(hit, 1.0, 0.0).reshape(experts * cap, tok).astype(BF16)


def one_hot_tokens(rank, cap):
    experts, tok = rank.shape
    lane = lax.broadcasted_iota(jnp.int32, (experts, experts * cap), 1)
    first = lax.broadcasted_iota(jnp.int32, (experts, experts * cap), 0) * cap
    mine = (lane >= first) & (lane < first + cap)
    spread = dot_tn(rank.astype(BF16), jnp.where(mine, 1.0, 0.0).astype(BF16))
    row = lax.broadcasted_iota(jnp.int32, (1, experts * cap), 1)
    for e in range(1, experts):
        row = row - jnp.where(lane[0:1] >= e * cap, cap, 0)
    return jnp.where(spread == row.astype(F32), 1.0, 0.0).astype(BF16)


def split3(x):
    hi = x.astype(BF16)
    rest = x - hi.astype(F32)
    mid = rest.astype(BF16)
    low = (rest - mid.astype(F32)).astype(BF16)
    return jnp.concatenate([hi, mid, low], axis=0)


def gather_kernel(u_ref, dy_ref, ids_ref, wr_ref, x_ref, d_ref, uall_ref, rank_ref, g_ref, prob_ref, gown_ref, cnt_ref,
                  rcv, pbuf, xbuf, in_sem, send_sem, recv_sem, tail_recv, meta_send, meta_recv, out_sem, uout_sem):
    y, c, z = position()
    me = block_of(y, c, z)
    tok = u_ref.shape[0]
    d_model = u_ref.shape[1]
    experts = wr_ref.shape[0]
    local = rank_ref.shape[1]
    cap = pbuf.shape[0] // local
    blocks = rcv.shape[1]

    own_u = pltpu.make_async_copy(u_ref, rcv.at[0, me], in_sem.at[0])
    own_d = pltpu.make_async_copy(dy_ref, rcv.at[1, me], in_sem.at[1])
    own_u.start()
    own_d.start()

    def rdma(arr, s, kind, ep_to, z_to):
        return pltpu.make_async_remote_copy(
            src_ref=rcv.at[arr, s], dst_ref=rcv.at[arr, s], send_sem=send_sem.at[arr, s, kind],
            recv_sem=recv_sem.at[arr, s], device_id={"ep": ep_to, "etp": z_to}, device_id_type=MESH)

    ep_sib = y * 2 + 1 - c
    ep_y = (1 - y) * 2 + c
    ep_me = y * 2 + c

    def send_down(arr, s):
        return rdma(arr, s, 0, ep_me, jnp.maximum(z - 1, 0))

    def send_up(arr, s):
        return rdma(arr, s, 1, ep_me, jnp.minimum(z + 1, 3))

    def send_y(arr, s):
        return rdma(arr, s, 2, ep_y, z)

    def send_sib(arr, s):
        return rdma(arr, s, 3, ep_sib, z)

    def part(arr, s, kind, ep_to, z_to, rows, sem):
        return pltpu.make_async_remote_copy(
            src_ref=rcv.at[arr, s, rows], dst_ref=rcv.at[arr, s, rows], send_sem=send_sem.at[arr, s, kind],
            recv_sem=sem.at[arr, s], device_id={"ep": ep_to, "etp": z_to}, device_id_type=MESH)

    head = pl.ds(0, tok - TAIL)
    tail = pl.ds(tok - TAIL, TAIL)

    def head_y(arr, s):
        return part(arr, s, 2, ep_y, z, head, recv_sem)

    def tail_down(arr, s):
        return part(arr, s, 0, ep_me, jnp.maximum(z - 1, 0), tail, tail_recv)

    def tail_up(arr, s):
        return part(arr, s, 1, ep_me, jnp.minimum(z + 1, 3), tail, tail_recv)

    for arr, own in ((0, own_u), (1, own_d)):
        own.wait()

        @pl.when(z > 0)
        def _():
            send_down(arr, me).start()

        @pl.when(z < 3)
        def _():
            send_up(arr, me).start()

        send_y(arr, me).start()
        send_sib(arr, me).start()

    logits = dot_nt(wr_ref[...], rcv[0, me])
    shifted = jnp.exp(logits - jnp.max(logits, axis=0, keepdims=True))
    prob = shifted / jnp.sum(shifted, axis=0, keepdims=True)
    expert_row = lax.broadcasted_iota(jnp.int32, (experts, tok), 0)
    chosen = expert_row == ids_ref[0:1, :]
    for j in range(1, ids_ref.shape[0]):
        chosen = chosen | (expert_row == ids_ref[j:j + 1, :])
    prob_ref[...] = jnp.zeros(prob_ref.shape, F32)
    prob_ref[:, 0:tok] = prob
    gown_ref[...] = jnp.full(gown_ref.shape, -1.0, F32)
    gown_ref[:, 0:tok] = jnp.where(chosen, prob, -1.0)
    g_ref[me] = gown_ref[pl.ds(pl.multiple_of(ep_me * local, local), local), :]

    def meta_copy(s):
        ep_to = s // 4
        return pltpu.make_async_remote_copy(
            src_ref=gown_ref.at[pl.ds(pl.multiple_of(ep_to * local, local), local), :], dst_ref=g_ref.at[me],
            send_sem=meta_send.at[s], recv_sem=meta_recv.at[me], device_id={"ep": ep_to, "etp": s % 4},
            device_id_type=MESH)

    def meta_wait(s):
        return pltpu.make_async_remote_copy(
            src_ref=gown_ref.at[pl.ds(0, local), :], dst_ref=g_ref.at[s], send_sem=meta_send.at[s],
            recv_sem=meta_recv.at[s], device_id={"ep": ep_me, "etp": z}, device_id_type=MESH)

    @pl.loop(1, blocks)
    def _(i):
        meta_copy((me + i) % blocks).start()

    lower = (lax.broadcasted_iota(jnp.int32, (LANES, LANES), 0) < lax.broadcasted_iota(jnp.int32, (LANES, LANES), 1))
    before = jnp.where(lower, 1.0, 0.0).astype(BF16)

    def out_copy(arr_is_dy, slot, s):
        return pltpu.make_async_copy(xbuf.at[slot], (d_ref if arr_is_dy else x_ref).at[s], out_sem.at[slot])

    def u_copy(s):
        return pltpu.make_async_copy(rcv.at[0, s], uall_ref.at[s], uout_sem.at[s])

    @pl.loop(0, 9)
    def _(t):
        turn = jnp.maximum(t - 1, 0)
        arr_t = turn % 2
        q_col = 1 + turn // 2
        q_y = turn // 2

        @pl.when((t >= 1) & (t <= 6))
        def _():
            zb = near_order(z, q_col)
            s = block_of(y, c, zb)
            send_y(arr_t, s).wait_recv()

            @pl.when((zb < z) & (z < 3))
            def _():
                send_up(arr_t, s).start()

            @pl.when((zb > z) & (z > 0))
            def _():
                send_down(arr_t, s).start()

            head_y(arr_t, s).start()
            send_sib(arr_t, s).start()

        @pl.when(t >= 1)
        def _():
            zb = near_order(z, q_y)
            s = block_of(1 - y, c, zb)

            @pl.when(q_y == 0)
            def _():
                send_y(arr_t, s).wait_recv()

            @pl.when(q_y > 0)
            def _():
                tail_up(arr_t, s).wait_recv()

            @pl.when((zb <= z) & (z < 3))
            def _():
                tail_up(arr_t, s).start()

            @pl.when((zb >= z) & (z > 0))
            def _():
                tail_down(arr_t, s).start()

            @pl.when(q_y > 0)
            def _():
                head_y(arr_t, s).wait_recv()

            send_sib(arr_t, s).start()

        @pl.loop(jnp.where(t > 6, 2, 0), 4)
        def _(i):
            flip = i % 2
            slot = flip
            typ = jnp.where(t == 0, 0, i // 2)
            arr = jnp.where(t == 0, i // 2, arr_t)
            core = c + flip - 2 * c * flip
            zb = near_order(z, jnp.where(t == 0, 0, jnp.where(typ == 0, q_col, q_y)))
            yb = y + typ - 2 * y * typ
            s = block_of(yb, core, zb)

            @pl.when(flip == 1)
            def _():
                send_y(arr, s).wait_recv()

            @pl.when(arr == 0)
            def _():
                u_copy(s).start()

                @pl.when(s != me)
                def _():
                    meta_wait(s).wait_recv()

                mask = g_ref[s] >= 0.0
                ones = jnp.where(mask, 1.0, 0.0)
                rank = dot_nn(ones.astype(BF16), before)
                held = dot_nt(jnp.ones(ones.shape, BF16), ones.astype(BF16))
                cnt_ref[pl.ds(s, 1), 0:local] = held[0:1, :].astype(jnp.int32)
                rank_ref[s] = jnp.where(mask, rank, -1.0)

            pbuf[...] = one_hot_slots(rank_ref[s][:, 0:tok], cap)

            @pl.when((t > 0) | (i >= 2))
            def _():
                out_copy(False, slot, s).wait()

            @pl.loop(0, d_model // CHUNK)
            def _(n):
                cols = pl.ds(pl.multiple_of(n * CHUNK, CHUNK), CHUNK)
                xbuf[slot, :, :, :, cols] = dot_nn(pbuf[...], rcv[arr, s, :, cols]).astype(BF16).reshape(xbuf.shape[1:4] + (CHUNK,))

            @pl.when(arr == 0)
            def _():
                out_copy(False, slot, s).start()

            @pl.when(arr == 1)
            def _():
                out_copy(True, slot, s).start()

    for slot in (0, 1):
        out_copy(False, slot, me).wait()

    @pl.loop(0, blocks)
    def _(s):
        u_copy(s).wait()

        @pl.when(s != me)
        def _():
            meta_copy(s).wait_send()

    @pl.loop(0, 4)
    def _(q):
        zb = near_order(z, q)
        s = block_of(y, c, zb)
        sy = block_of(1 - y, c, zb)
        for arr in (0, 1):
            @pl.when((z > 0) & (zb >= z))
            def _():
                send_down(arr, s).wait_send()
                tail_down(arr, sy).wait_send()

            @pl.when((z < 3) & (zb <= z))
            def _():
                send_up(arr, s).wait_send()
                tail_up(arr, sy).wait_send()

            @pl.when(q == 0)
            def _():
                send_y(arr, s).wait_send()

            @pl.when(q > 0)
            def _():
                head_y(arr, s).wait_send()

            send_sib(arr, s).wait_send()
            send_sib(arr, sy).wait_send()


class ExpertTiles:
    def __init__(self, x_in, d_in, go, dx, wg, wu, wd, te, tk, tn, sg, xb, db, gob, dxb, wb, in_sem, out_sem, w_sem):
        self.te, self.tk, self.tn, self.sg = te, tk, tn, sg
        self.x_in, self.d_in, self.go, self.dx = x_in, d_in, go, dx
        self.w = (wg, wu, wd)
        self.xb, self.db, self.gob, self.dxb, self.wb = xb, db, gob, dxb, wb
        self.in_sem, self.out_sem, self.w_sem = in_sem, out_sem, w_sem

    def seg(self, ref, i, j):
        at = self.sg[i * HALF + j]
        return ref.at[at // 4, self.te[i], at % 4]

    def half(self, ref, i):
        return ref.at[pl.ds(pl.multiple_of(self.tk[i] * HALF, HALF), HALF), self.te[i], 0]

    def each(self, i, slot, act, moves, sem):
        @pl.when(self.tk[i] < 2)
        def _():
            for a, (hbm, buf, out) in enumerate(moves):
                ends = (buf.at[slot], self.half(hbm, i)) if out else (self.half(hbm, i), buf.at[slot])
                act(pltpu.make_async_copy(*ends, sem.at[a, slot, HALF]))

        for j in range(HALF):
            @pl.when((self.tk[i] == 2) & (j < self.tn[i]))
            def _():
                for a, (hbm, buf, out) in enumerate(moves):
                    ends = (buf.at[slot, j], self.seg(hbm, i, j)) if out else (self.seg(hbm, i, j), buf.at[slot, j])
                    act(pltpu.make_async_copy(*ends, sem.at[a, slot, j]))

    def load(self, i, slot, act):
        self.each(i, slot, act, ((self.x_in, self.xb, False), (self.d_in, self.db, False)), self.in_sem)

    def store(self, i, slot, act):
        self.each(i, slot, act, ((self.go, self.gob, True), (self.dx, self.dxb, True)), self.out_sem)

    def weights(self, e, p):
        return [pltpu.make_async_copy(src.at[e], self.wb.at[p, j], self.w_sem.at[p, j]) for j, src in enumerate(self.w)]

    def run(self, i, slot, p, fresh, dwb, dob, sgb, rank_ref, g_ref, dg_ref):
        rows = HALF * LEVEL_ROWS
        d_model = self.xb.shape[-1]
        one = pl.ds(self.te[i], 1)
        for j in range(HALF):
            at = self.sg[i * HALF + j]
            level = jnp.where(j < self.tn[i], at % 4, 8) * LEVEL_ROWS
            sgb[0, pl.ds(j, 1), :] = rank_ref[at // 4, one, :] - level.astype(F32)
            sgb[1, pl.ds(j, 1), :] = g_ref[at // 4, one, :]
        row = lax.broadcasted_iota(jnp.int32, (HALF, LEVEL_ROWS, LANES), 1)
        hit = sgb[0][:, None, :] == row.astype(F32)
        g_slot = jnp.sum(jnp.where(hit, sgb[1][:, None, :], 0.0), axis=2, keepdims=True).reshape(rows, 1)
        x = self.xb[slot].reshape(rows, d_model)
        h1 = dot_nt(x, self.wb[p, 0]).astype(BF16).astype(F32)
        h3 = dot_nt(x, self.wb[p, 1]).astype(BF16).astype(F32)
        sig = jax.nn.sigmoid(h1)
        silu = h1 * sig
        act = (silu * h3).astype(BF16)
        chunks = [slice(n, n + CHUNK) for n in range(0, d_model, CHUNK)]
        dg = jnp.zeros((rows, 1), F32)
        da = jnp.zeros((rows, act.shape[1]), F32)
        for cols in chunks:
            out = dot_nn(act, self.wb[p, 2, :, cols])
            dy = self.db[slot, :, :, cols].reshape(rows, CHUNK).astype(F32)
            dg = dg + jnp.sum(out * dy, axis=1, keepdims=True)
            self.gob[slot, :, :, cols] = (out * g_slot).astype(BF16).reshape(HALF, LEVEL_ROWS, CHUNK)
            do = (dy * g_slot).astype(BF16)
            dob[:, cols] = do
            da = da + dot_nt(do, self.wb[p, 2, :, cols])
        da = da.astype(BF16).astype(F32)
        dh1 = (da * h3 * sig * (1.0 + h1 * (1.0 - sig))).astype(BF16)
        dh3 = (da * silu).astype(BF16)
        for cols in chunks:
            dx = dot_nn(dh1, self.wb[p, 0, :, cols]) + dot_nn(dh3, self.wb[p, 1, :, cols])
            self.dxb[slot, :, :, cols] = dx.astype(BF16).reshape(HALF, LEVEL_ROWS, CHUNK)
        sgb[0] = jnp.sum(jnp.where(hit, dg.reshape(HALF, LEVEL_ROWS, 1), 0.0), axis=1)
        for j in range(HALF):
            dg_ref[self.sg[i * HALF + j] // 4, one, :] += sgb[0, pl.ds(j, 1), :]

        def add_dw(first):
            for cols in chunks:
                xc = self.xb[slot, :, :, cols].reshape(rows, CHUNK)
                for j, (left, right) in enumerate(((dh1, xc), (dh3, xc), (act, dob[:, cols]))):
                    part = dot_tn(left, right)
                    dwb[p, j, :, cols] = part if first else dwb[p, j, :, cols] + part

        @pl.when(fresh)
        def _():
            add_dw(True)

        @pl.when(jnp.logical_not(fresh))
        def _():
            add_dw(False)


def expert_kernel(cnt, x_hbm, d_hbm, wg_hbm, wu_hbm, wd_hbm, rank_ref, g_ref, go_hbm, dx_hbm, dwg_hbm, dwu_hbm, dwd_hbm, dg_ref,
                  te, tk, tn, sg, xb, db, gob, dxb, wb, dwb, dob, sgb, in_sem, out_sem, w_sem, dw_sem):
    local = wg_hbm.shape[0]
    levels = x_hbm.shape[2]
    blocks = x_hbm.shape[0]
    halves = blocks // HALF
    tiles = ExpertTiles(x_hbm, d_hbm, go_hbm, dx_hbm, wg_hbm, wu_hbm, wd_hbm, te, tk, tn, sg, xb, db, gob, dxb, wb, in_sem, out_sem, w_sem)

    def start(copy):
        copy.start()

    def wait(copy):
        copy.wait()

    def dw_out(e, p):
        return [pltpu.make_async_copy(dwb.at[p, j], dst.at[e], dw_sem.at[p, j]) for j, dst in enumerate((dwg_hbm, dwu_hbm, dwd_hbm))]

    te[0] = 0
    tk[0] = 0
    tn[0] = HALF
    for copy in tiles.weights(0, 0):
        copy.start()
    tiles.load(0, 0, start)
    dg_ref[...] = jnp.zeros(dg_ref.shape, F32)

    def add_expert(e, n):
        for h in range(halves):
            te[n + h] = e
            tk[n + h] = h
            tn[n + h] = HALF
            for j in range(HALF):
                sg[(n + h) * HALF + j] = (h * HALF + j) * 4
        n = n + halves

        def add_block(b, m):
            held = cnt[b, e]
            for level in range(1, levels):
                sg[n * HALF + m] = b * 4 + level
                m = m + jnp.where(held > level * LEVEL_ROWS, 1, 0)
            return m

        m = lax.fori_loop(0, blocks, add_block, 0)
        for j in range(HALF):
            sg[n * HALF + m + j] = 0
        extra = (m + HALF - 1) // HALF

        def add_tile(k, carry):
            te[n + k] = e
            tk[n + k] = 2
            tn[n + k] = jnp.minimum(m - k * HALF, HALF)
            return carry

        lax.fori_loop(0, extra, add_tile, 0)
        return n + extra

    count = lax.fori_loop(0, local, add_expert, 0)
    te[count] = local

    def step(i, carry):
        slot = i % 2
        e = te[i]
        p = e % 2
        fresh = (i == 0) | (te[jnp.maximum(i - 1, 0)] != e)
        last = te[i + 1] != e

        @pl.when(i + 1 < count)
        def _():
            tiles.load(i + 1, 1 - slot, start)

        @pl.when(fresh)
        def _():
            @pl.when(e + 1 < local)
            def _():
                for copy in tiles.weights(e + 1, 1 - p):
                    copy.start()

            for copy in tiles.weights(e, p):
                copy.wait()

            @pl.when(e >= 2)
            def _():
                for copy in dw_out(e, p):
                    copy.wait()

        tiles.load(i, slot, wait)

        @pl.when(i >= 2)
        def _():
            tiles.store(i - 2, slot, wait)

        tiles.run(i, slot, p, fresh, dwb, dob, sgb, rank_ref, g_ref, dg_ref)
        tiles.store(i, slot, start)

        @pl.when(last)
        def _():
            for copy in dw_out(e, p):
                copy.start()

        return carry

    lax.fori_loop(0, count, step, 0)
    for p in (0, 1):
        i = count - 2 + p
        tiles.store(i, i % 2, wait)
        for copy in dw_out(0, p):
            copy.wait()


def scatter_kernel(go_ref, dx_ref, uall_ref, rank_ref, dgb_ref, prob_ref, gown_ref, u_ref, dy_ref, wr_ref,
                   yo_ref, du_ref, dwr_ref,
                   slots, pbuf, acc, sib_out, sib_in, y_out, y_in, z_out, z_in, dg_in, dl_all, ubuf,
                   ld_sem, sib_ss, sib_rs, y_ss, y_rs, z_ss, z_rs, dg_ss, dg_rs, dl_ss, dl_rs, u_sem):
    y, c, z = position()
    me = block_of(y, c, z)
    ep_me = y * 2 + c
    ep_sib = y * 2 + 1 - c
    ep_y = (1 - y) * 2 + c
    blocks, local, lanes = rank_ref.shape
    tok, d_model = u_ref.shape
    cap = pbuf.shape[1] // local
    experts = prob_ref.shape[0]

    def dg_copy(s, src):
        return pltpu.make_async_remote_copy(
            src_ref=dgb_ref.at[s], dst_ref=dg_in.at[src], send_sem=dg_ss.at[s], recv_sem=dg_rs.at[src],
            device_id={"ep": s // 4, "etp": s % 4}, device_id_type=MESH)

    def dl_copy(s, src):
        return pltpu.make_async_remote_copy(
            src_ref=dl_all.at[src], dst_ref=dl_all.at[src], send_sem=dl_ss.at[s], recv_sem=dl_rs.at[src],
            device_id={"ep": s // 4, "etp": s % 4}, device_id_type=MESH)

    def sib_copy(slot, arr, k):
        return pltpu.make_async_remote_copy(
            src_ref=sib_out.at[slot], dst_ref=sib_in.at[arr, k], send_sem=sib_ss.at[slot], recv_sem=sib_rs.at[arr, k],
            device_id={"ep": ep_sib, "etp": z}, device_id_type=MESH)

    def y_copy(arr, k):
        return pltpu.make_async_remote_copy(
            src_ref=y_out.at[arr, k], dst_ref=y_in.at[arr, k], send_sem=y_ss.at[arr, k], recv_sem=y_rs.at[arr, k],
            device_id={"ep": ep_y, "etp": z}, device_id_type=MESH)

    def z_copy(arr, k, slot, z_to):
        return pltpu.make_async_remote_copy(
            src_ref=z_out.at[arr, k], dst_ref=z_in.at[arr, slot], send_sem=z_ss.at[arr, k], recv_sem=z_rs.at[arr, slot],
            device_id={"ep": ep_me, "etp": z_to}, device_id_type=MESH)

    def plan(n):
        group = (n - 12) // 3
        rest = (n - 12) % 3
        mid = (n >= 12) & (n < 21)
        arr = jnp.where((n < 12) | (n == 23) | (mid & (rest == 0)), 0, 1)
        phase = jnp.where(n < 8, 1, jnp.where(n < 12, 2, jnp.where(n < 21, jnp.where(rest == 0, 3, 1), jnp.where(n < 23, 1, jnp.where(n == 23, 3, jnp.where(n < 28, 2, 3))))))
        sub = jnp.where(n < 8, n % 2, jnp.where(n < 21, rest - 1, n - 21))
        k = jnp.where(n < 8, n // 2, jnp.where(n < 12, n - 8, jnp.where(n < 21, group, jnp.where(n < 24, 3, n % 4))))
        to_sib = jnp.where(phase == 1, 1 - sub, jnp.where(phase == 2, 1, 0))
        other = jnp.where(phase == 1, 1, 0)
        core = c + to_sib - 2 * c * to_sib
        col = y + other - 2 * y * other
        return arr, phase, k, to_sib, block_of(col, core, far_order(z, k))

    def start_load(n, slot):
        arr, phase, k, to_sib, s = plan(n)

        @pl.when(arr == 0)
        def _():
            pltpu.make_async_copy(go_ref.at[s], slots.at[slot], ld_sem.at[slot]).start()

        @pl.when(arr == 1)
        def _():
            pltpu.make_async_copy(dx_ref.at[s], slots.at[slot], ld_sem.at[slot]).start()

    start_load(0, 0)

    @pl.loop(1, blocks)
    def _(i):
        dg_copy((me + i) % blocks, me).start()

    dg_in[me] = dgb_ref[me]
    dwr_ref[...] = jnp.zeros(dwr_ref.shape, F32)

    def u_load(b):
        return pltpu.make_async_copy(uall_ref.at[b], ubuf.at[b % 2], u_sem.at[b % 2])

    @pl.loop(0, 32)
    def _(n):
        slot = n % 2
        arr, phase, k, to_sib, s = plan(n)

        @pl.when(n < 31)
        def _():
            start_load(n + 1, 1 - slot)

        pbuf[...] = one_hot_tokens(rank_ref[s][:, 0:tok], cap)
        pltpu.make_async_copy(go_ref.at[s], slots.at[slot], ld_sem.at[slot]).wait()

        @pl.loop(0, d_model // CHUNK)
        def _(m):
            cols = pl.ds(pl.multiple_of(m * CHUNK, CHUNK), CHUNK)
            acc[:, cols] = dot_nn(pbuf[...], slots[slot, :, cols])

        @pl.when(to_sib == 1)
        def _():
            idx = k + 4 * (phase - 1)
            out = idx % 2

            @pl.when((idx >= 2) | (arr == 1))
            def _():
                sib_copy(out, arr, idx).wait_send()

            sib_out[out] = acc[...].astype(BF16)
            sib_copy(out, arr, idx).start()

        @pl.when((phase == 1) & (to_sib == 0))
        def _():
            sib_copy(0, arr, k).wait_recv()
            y_out[arr, k] = (acc[...] + sib_in[arr, k].astype(F32)).astype(BF16)
            y_copy(arr, k).start()

        @pl.when(phase == 3)
        def _():
            sib_copy(0, arr, k + 4).wait_recv()
            y_copy(arr, k).wait_recv()
            acc[...] = acc[...] + sib_in[arr, k + 4].astype(F32) + y_in[arr, k].astype(F32)
            target = far_order(z, k)

            @pl.when(((target > z) & (z > 0)) | ((target < z) & (z < 3)) | ((target == z) & (z > 0)))
            def _():
                z_copy(arr, 0, target, z).wait_recv()
                acc[...] += z_in[arr, target].astype(F32)

            @pl.when((target == z) & (z < 3))
            def _():
                z_copy(arr, 0, 4, z).wait_recv()
                acc[...] += z_in[arr, 4].astype(F32)

            @pl.when(k < 3)
            def _():
                z_out[arr, k] = acc[...].astype(BF16)
                z_to = jnp.where(target > z, z + 1, z - 1)
                dst = jnp.where(target == z - 1, 4, target)
                z_copy(arr, k, dst, z_to).start()

            @pl.when((k == 3) & (arr == 0))
            def _():
                yo_ref[...] = (u_ref[...].astype(F32) + acc[...]).astype(BF16)

            @pl.when((k == 3) & (arr == 1))
            def _():
                dl3 = split3(dl_all[me][:, 0:tok])
                wr = wr_ref[...]
                router = dot_tn(dl3, jnp.concatenate([wr, wr, wr], axis=0))
                du_ref[...] = (dy_ref[...].astype(F32) + acc[...] + router).astype(BF16)

        @pl.when(n == 1)
        def _():
            @pl.loop(0, blocks)
            def _(b):
                @pl.when(b != me)
                def _():
                    dg_copy(me, b).wait_recv()

            d_gate = jnp.sum(dg_in[...].reshape(4, 4, local, lanes), axis=1).reshape(experts, lanes)
            d_prob = jnp.where(gown_ref[...] >= 0.0, d_gate, 0.0)
            prob = prob_ref[...]
            dl_all[me] = prob * (d_prob - jnp.sum(prob * d_prob, axis=0, keepdims=True))

            @pl.loop(1, blocks)
            def _(b):
                dl_copy((me + b) % blocks, me).start()

        @pl.when((n >= 15) & (n < 31))
        def _():
            u_load(n - 15).start()

        @pl.when(n >= 16)
        def _():
            b = n - 16

            @pl.when(b != me)
            def _():
                dl_copy(me, b).wait_recv()

            u_load(b).wait()
            part = dot_nn(split3(dl_all[b][:, 0:tok]), ubuf[b % 2])
            dwr_ref[...] += part[0:experts] + part[experts:2 * experts] + part[2 * experts:3 * experts]

    for out in (0, 1):
        sib_copy(out, 0, 0).wait_send()

    @pl.loop(0, 4)
    def _(k):
        for arr in (0, 1):
            y_copy(arr, k).wait_send()

            @pl.when(k < 3)
            def _():
                z_copy(arr, k, 0, z).wait_send()

    @pl.loop(0, blocks)
    def _(b):
        @pl.when(b != me)
        def _():
            dg_copy(b, me).wait_send()
            dl_copy(b, me).wait_send()


def solution(mesh):
    ep_size = mesh.shape["ep"]
    etp_size = mesh.shape["etp"]
    blocks = ep_size * etp_size
    tok_spec = P(("dp", "ep", "etp"), None)
    col_spec = P("ep", None, "etp")
    row_spec = P("ep", "etp", None)
    in_specs = (tok_spec, tok_spec, tok_spec, P(None, None), col_spec, col_spec, row_spec)
    out_specs = (tok_spec, tok_spec, P(("dp", "ep"), None, "etp"), P(("dp", "ep"), None, "etp"), P(("dp", "ep"), "etp", None), P("dp", None))
    any_spec = pl.BlockSpec(memory_space=pl.ANY)
    vmem = pl.BlockSpec(memory_space=pltpu.VMEM)
    dma = pltpu.SemaphoreType.DMA

    def device_step(u_loc, dy_loc, ids_loc, w_router, w_gate, w_up, w_down):
        tok, d_model = u_loc.shape
        top_k = ids_loc.shape[1]
        experts = w_router.shape[1]
        local = w_gate.shape[0]
        ffn = w_gate.shape[2]
        cap = 96
        slots = local * cap
        ids_t = ids_loc.T
        wr_t = w_router.T
        wg_t = jnp.swapaxes(w_gate, 1, 2)
        wu_t = jnp.swapaxes(w_up, 1, 2)

        levels = cap // LEVEL_ROWS
        tile_shape = jax.ShapeDtypeStruct((blocks, local, levels, LEVEL_ROWS, d_model), BF16)
        dw_shape = jax.ShapeDtypeStruct((local, ffn, d_model), F32)
        meta_shape = jax.ShapeDtypeStruct((blocks, local, LANES), F32)
        own_shape = jax.ShapeDtypeStruct((experts, LANES), F32)
        tile_buf = pltpu.VMEM((2, HALF, LEVEL_ROWS, d_model), BF16)
        weight_buf = pltpu.VMEM((2, 3, ffn, d_model), BF16)
        x_slots, d_slots, u_all, rank, gate, prob, g_own, counts = pl.pallas_call(
            gather_kernel,
            name="gather",
            out_shape=(tile_shape, tile_shape, jax.ShapeDtypeStruct((blocks, tok, d_model), BF16), meta_shape, meta_shape, own_shape, own_shape,
                       jax.ShapeDtypeStruct((blocks, 128), jnp.int32)),
            in_specs=[any_spec, any_spec, vmem, vmem],
            out_specs=(any_spec, any_spec, any_spec, vmem, vmem, vmem, vmem, vmem),
            scratch_shapes=[
                pltpu.VMEM((2, blocks, tok, d_model), BF16),
                pltpu.VMEM((slots, tok), BF16),
                pltpu.VMEM((2, local, levels, LEVEL_ROWS, d_model), BF16),
                dma((2,)), dma((2, blocks, 4)), dma((2, blocks)), dma((2, blocks)), dma((blocks,)), dma((blocks,)), dma((2,)), dma((blocks,)),
            ],
            compiler_params=pltpu.CompilerParams(has_side_effects=True, vmem_limit_bytes=60 * 1024 * 1024),
        )(u_loc, dy_loc, ids_t, wr_t)

        max_tiles = local * levels * (blocks // HALF) + 8
        smem_list = pltpu.SMEM((max_tiles,), jnp.int32)
        smem = pl.BlockSpec(memory_space=pltpu.SMEM)
        go, dx, dwg, dwu, dwd, dg_blocks = pl.pallas_call(
            expert_kernel,
            name="experts",
            out_shape=(tile_shape, tile_shape, dw_shape, dw_shape, dw_shape, meta_shape),
            in_specs=[smem] + [any_spec] * 5 + [vmem] * 2,
            out_specs=(any_spec,) * 5 + (vmem,),
            scratch_shapes=[
                smem_list, smem_list, smem_list, pltpu.SMEM((max_tiles * HALF,), jnp.int32), tile_buf, tile_buf, tile_buf, tile_buf, weight_buf,
                pltpu.VMEM((2, 3, ffn, d_model), F32),
                pltpu.VMEM((HALF * LEVEL_ROWS, d_model), BF16),
                pltpu.VMEM((2, HALF, LANES), F32),
                dma((2, 2, HALF + 1)), dma((2, 2, HALF + 1)), dma((2, 3)), dma((2, 3)),
            ],
            input_output_aliases={1: 0, 2: 1},
            compiler_params=pltpu.CompilerParams(vmem_limit_bytes=60 * 1024 * 1024),
        )(counts, x_slots, d_slots, wg_t, wu_t, w_down, rank, gate)

        slot_shape = (blocks, slots, d_model)
        y_loc, du_loc, dwr_t = pl.pallas_call(
            scatter_kernel,
            name="scatter",
            out_shape=(jax.ShapeDtypeStruct((tok, d_model), BF16), jax.ShapeDtypeStruct((tok, d_model), BF16), jax.ShapeDtypeStruct((experts, d_model), F32)),
            in_specs=[any_spec, any_spec, any_spec] + [vmem] * 7,
            out_specs=(vmem, vmem, vmem),
            scratch_shapes=[
                pltpu.VMEM((2, slots, d_model), BF16),
                pltpu.VMEM((tok, slots), BF16),
                pltpu.VMEM((tok, d_model), F32),
                pltpu.VMEM((2, tok, d_model), BF16),
                pltpu.VMEM((2, 8, tok, d_model), BF16),
                pltpu.VMEM((2, 4, tok, d_model), BF16),
                pltpu.VMEM((2, 4, tok, d_model), BF16),
                pltpu.VMEM((2, 3, tok, d_model), BF16),
                pltpu.VMEM((2, 5, tok, d_model), BF16),
                pltpu.VMEM((blocks, local, LANES), F32),
                pltpu.VMEM((blocks, experts, LANES), F32),
                pltpu.VMEM((2, tok, d_model), BF16),
                dma((2,)), dma((2,)), dma((2, 8)), dma((2, 4)), dma((2, 4)), dma((2, 3)), dma((2, 5)),
                dma((blocks,)), dma((blocks,)), dma((blocks,)), dma((blocks,)), dma((2,)),
            ],
            compiler_params=pltpu.CompilerParams(has_side_effects=True, vmem_limit_bytes=60 * 1024 * 1024),
        )(go.reshape(slot_shape), dx.reshape(slot_shape), u_all, rank, dg_blocks, prob, g_own, u_loc, dy_loc, wr_t)

        dw_gate = jnp.swapaxes(dwg, 1, 2)
        dw_up = jnp.swapaxes(dwu, 1, 2)
        return y_loc, du_loc, dw_gate, dw_up, dwd, dwr_t.T

    return jax.shard_map(device_step, mesh=mesh, in_specs=in_specs, out_specs=out_specs, check_vma=False)
```

```python
import jax
import jax.numpy as jnp
from jax import lax
from jax.experimental import pallas as pl
from jax.experimental.pallas import tpu as pltpu
from jax.sharding import PartitionSpec as P

MESH = pl.DeviceIdType.MESH
F32 = jnp.float32
BF16 = jnp.bfloat16
LANES = 256
LEVEL_ROWS = 32
HALF = 8
CHUNK = 512
EXPERT_CHUNK = 256
TAIL = 16
PAIR = (0, 1)
VMEM_LIMIT = 60 * 1024 * 1024


def dot_nn(a, b):
    return lax.dot_general(a, b, (((1,), (0,)), ((), ())), preferred_element_type=F32)


def dot_nt(a, b):
    return lax.dot_general(a, b, (((1,), (1,)), ((), ())), preferred_element_type=F32)


def dot_tn(a, b):
    return lax.dot_general(a, b, (((0,), (0,)), ((), ())), preferred_element_type=F32)


def position():
    ep = lax.axis_index("ep")
    z = lax.axis_index("etp")
    return ep // 2, ep % 2, z


def flipped(a):
    return 1 - a


def swap(a, b):
    return a + b - 2 * a * b


def ep_of(y, c):
    return y * 2 + c


def device_of(s):
    return {"ep": s // 4, "etp": s % 4}


def as_one(hit):
    return jnp.where(hit, 1.0, 0.0)


def block_of(y, c, z):
    return ep_of(y, c) * 4 + z


def near_order(z, q):
    near = z - 1 + 2 * (1 - jnp.minimum(z, 1))
    far = 3 * (1 - z // 2)
    third = 6 - z - near - far
    return jnp.where(q == 0, z, jnp.where(q == 1, near, jnp.where(q == 2, third, far)))


def far_order(z, k):
    first = 3 * (1 - z // 2)
    second = (2 + 3 * z) % 5
    third = 1 + z % 2
    return jnp.where(k == 0, first, jnp.where(k == 1, second, jnp.where(k == 2, third, z)))


def one_hot_slots(rank, cap):
    tok = rank.shape[1]
    experts = rank.shape[0]
    row = lax.broadcasted_iota(jnp.int32, (experts, cap, tok), 1).astype(F32)
    hit = rank[:, None, :] == row
    return as_one(hit).reshape(experts * cap, tok).astype(BF16)


def one_hot_tokens(rank, cap):
    experts, tok = rank.shape
    lane = lax.broadcasted_iota(jnp.int32, (experts, experts * cap), 1)
    first = lax.broadcasted_iota(jnp.int32, (experts, experts * cap), 0) * cap
    mine = (lane >= first) & (lane < first + cap)
    spread = dot_tn(rank.astype(BF16), as_one(mine).astype(BF16))
    row = lax.broadcasted_iota(jnp.int32, (1, experts * cap), 1)
    for e in range(1, experts):
        row = row - jnp.where(lane[0:1] >= e * cap, cap, 0)
    return as_one(spread == row.astype(F32)).astype(BF16)


def split3(x):
    hi = x.astype(BF16)
    rest = x - hi.astype(F32)
    mid = rest.astype(BF16)
    low = (rest - mid.astype(F32)).astype(BF16)
    return jnp.concatenate([hi, mid, low], axis=0)


def gather_kernel(u_ref, dy_ref, ids_ref, wr_ref, x_ref, d_ref, uall_ref, rank_ref, g_ref, prob_ref, gown_ref, cnt_ref,
                  rcv, pbuf, xbuf, in_sem, send_sem, recv_sem, tail_recv, meta_send, meta_recv, out_sem, uout_sem):
    y, c, z = position()
    me = block_of(y, c, z)
    tok = u_ref.shape[0]
    d_model = u_ref.shape[1]
    experts = wr_ref.shape[0]
    local = rank_ref.shape[1]
    cap = pbuf.shape[0] // local
    blocks = rcv.shape[1]

    own_u = pltpu.make_async_copy(u_ref, rcv.at[0, me], in_sem.at[0])
    own_d = pltpu.make_async_copy(dy_ref, rcv.at[1, me], in_sem.at[1])
    own_u.start()
    own_d.start()

    def rdma(arr, s, kind, ep_to, z_to):
        return pltpu.make_async_remote_copy(
            src_ref=rcv.at[arr, s], dst_ref=rcv.at[arr, s], send_sem=send_sem.at[arr, s, kind],
            recv_sem=recv_sem.at[arr, s], device_id={"ep": ep_to, "etp": z_to}, device_id_type=MESH)

    ep_sib = ep_of(y, flipped(c))
    ep_y = ep_of(flipped(y), c)
    ep_me = ep_of(y, c)

    def send_down(arr, s):
        return rdma(arr, s, 0, ep_me, jnp.maximum(z - 1, 0))

    def send_up(arr, s):
        return rdma(arr, s, 1, ep_me, jnp.minimum(z + 1, 3))

    def send_y(arr, s):
        return rdma(arr, s, 2, ep_y, z)

    def send_sib(arr, s):
        return rdma(arr, s, 3, ep_sib, z)

    def part(arr, s, kind, ep_to, z_to, rows, sem):
        return pltpu.make_async_remote_copy(
            src_ref=rcv.at[arr, s, rows], dst_ref=rcv.at[arr, s, rows], send_sem=send_sem.at[arr, s, kind],
            recv_sem=sem.at[arr, s], device_id={"ep": ep_to, "etp": z_to}, device_id_type=MESH)

    head = pl.ds(0, tok - TAIL)
    tail = pl.ds(tok - TAIL, TAIL)

    def head_y(arr, s):
        return part(arr, s, 2, ep_y, z, head, recv_sem)

    def tail_down(arr, s):
        return part(arr, s, 0, ep_me, jnp.maximum(z - 1, 0), tail, tail_recv)

    def tail_up(arr, s):
        return part(arr, s, 1, ep_me, jnp.minimum(z + 1, 3), tail, tail_recv)

    for arr, own in ((0, own_u), (1, own_d)):
        own.wait()

        @pl.when(z > 0)
        def _():
            send_down(arr, me).start()

        @pl.when(z < 3)
        def _():
            send_up(arr, me).start()

        send_y(arr, me).start()
        send_sib(arr, me).start()

    logits = dot_nt(wr_ref[...], rcv[0, me])
    shifted = jnp.exp(logits - jnp.max(logits, axis=0, keepdims=True))
    prob = shifted / jnp.sum(shifted, axis=0, keepdims=True)
    expert_row = lax.broadcasted_iota(jnp.int32, (experts, tok), 0)
    chosen = expert_row == ids_ref[0:1, :]
    for j in range(1, ids_ref.shape[0]):
        chosen = chosen | (expert_row == ids_ref[j:j + 1, :])
    prob_ref[...] = jnp.zeros(prob_ref.shape, F32)
    prob_ref[:, 0:tok] = prob
    gown_ref[...] = jnp.full(gown_ref.shape, -1.0, F32)
    gown_ref[:, 0:tok] = jnp.where(chosen, prob, -1.0)
    g_ref[me] = gown_ref[pl.ds(pl.multiple_of(ep_me * local, local), local), :]

    def meta_copy(s):
        ep_to = s // 4
        return pltpu.make_async_remote_copy(
            src_ref=gown_ref.at[pl.ds(pl.multiple_of(ep_to * local, local), local), :], dst_ref=g_ref.at[me],
            send_sem=meta_send.at[s], recv_sem=meta_recv.at[me], device_id=device_of(s),
            device_id_type=MESH)

    def meta_wait(s):
        return pltpu.make_async_remote_copy(
            src_ref=gown_ref.at[pl.ds(0, local), :], dst_ref=g_ref.at[s], send_sem=meta_send.at[s],
            recv_sem=meta_recv.at[s], device_id={"ep": ep_me, "etp": z}, device_id_type=MESH)

    @pl.loop(1, blocks)
    def _(i):
        meta_copy((me + i) % blocks).start()

    lower = (lax.broadcasted_iota(jnp.int32, (LANES, LANES), 0) < lax.broadcasted_iota(jnp.int32, (LANES, LANES), 1))
    before = as_one(lower).astype(BF16)

    def out_copy(arr_is_dy, slot, s):
        return pltpu.make_async_copy(xbuf.at[slot], (d_ref if arr_is_dy else x_ref).at[s], out_sem.at[slot])

    def u_copy(s):
        return pltpu.make_async_copy(rcv.at[0, s], uall_ref.at[s], uout_sem.at[s])

    @pl.loop(0, 9)
    def _(t):
        turn = jnp.maximum(t - 1, 0)
        arr_t = turn % 2
        q_col = 1 + turn // 2
        q_y = turn // 2

        @pl.when((t >= 1) & (t <= 6))
        def _():
            zb = near_order(z, q_col)
            s = block_of(y, c, zb)
            send_y(arr_t, s).wait_recv()

            @pl.when((zb < z) & (z < 3))
            def _():
                send_up(arr_t, s).start()

            @pl.when((zb > z) & (z > 0))
            def _():
                send_down(arr_t, s).start()

            head_y(arr_t, s).start()
            send_sib(arr_t, s).start()

        @pl.when(t >= 1)
        def _():
            zb = near_order(z, q_y)
            s = block_of(flipped(y), c, zb)

            @pl.when(q_y == 0)
            def _():
                send_y(arr_t, s).wait_recv()

            @pl.when(q_y > 0)
            def _():
                tail_up(arr_t, s).wait_recv()

            @pl.when((zb <= z) & (z < 3))
            def _():
                tail_up(arr_t, s).start()

            @pl.when((zb >= z) & (z > 0))
            def _():
                tail_down(arr_t, s).start()

            @pl.when(q_y > 0)
            def _():
                head_y(arr_t, s).wait_recv()

            send_sib(arr_t, s).start()

        @pl.loop(jnp.where(t > 6, 2, 0), 4)
        def _(i):
            flip = i % 2
            slot = flip
            typ = jnp.where(t == 0, 0, i // 2)
            arr = jnp.where(t == 0, i // 2, arr_t)
            core = swap(c, flip)
            zb = near_order(z, jnp.where(t == 0, 0, jnp.where(typ == 0, q_col, q_y)))
            yb = swap(y, typ)
            s = block_of(yb, core, zb)

            @pl.when(flip == 1)
            def _():
                send_y(arr, s).wait_recv()

            @pl.when(arr == 0)
            def _():
                u_copy(s).start()

                @pl.when(s != me)
                def _():
                    meta_wait(s).wait_recv()

                mask = g_ref[s] >= 0.0
                ones = as_one(mask)
                rank = dot_nn(ones.astype(BF16), before)
                held = dot_nt(jnp.ones(ones.shape, BF16), ones.astype(BF16))
                cnt_ref[pl.ds(s, 1), 0:local] = held[0:1, :].astype(jnp.int32)
                rank_ref[s] = jnp.where(mask, rank, -1.0)

            pbuf[...] = one_hot_slots(rank_ref[s][:, 0:tok], cap)

            @pl.when((t > 0) | (i >= 2))
            def _():
                out_copy(False, slot, s).wait()

            @pl.loop(0, d_model // CHUNK)
            def _(n):
                cols = pl.ds(pl.multiple_of(n * CHUNK, CHUNK), CHUNK)
                xbuf[slot, :, :, :, cols] = dot_nn(pbuf[...], rcv[arr, s, :, cols]).astype(BF16).reshape(xbuf.shape[1:4] + (CHUNK,))

            @pl.when(arr == 0)
            def _():
                out_copy(False, slot, s).start()

            @pl.when(arr == 1)
            def _():
                out_copy(True, slot, s).start()

    for slot in PAIR:
        out_copy(False, slot, me).wait()

    @pl.loop(0, blocks)
    def _(s):
        u_copy(s).wait()

        @pl.when(s != me)
        def _():
            meta_copy(s).wait_send()

    @pl.loop(0, 4)
    def _(q):
        zb = near_order(z, q)
        s = block_of(y, c, zb)
        sy = block_of(flipped(y), c, zb)
        for arr in PAIR:
            @pl.when((z > 0) & (zb >= z))
            def _():
                send_down(arr, s).wait_send()
                tail_down(arr, sy).wait_send()

            @pl.when((z < 3) & (zb <= z))
            def _():
                send_up(arr, s).wait_send()
                tail_up(arr, sy).wait_send()

            @pl.when(q == 0)
            def _():
                send_y(arr, s).wait_send()

            @pl.when(q > 0)
            def _():
                head_y(arr, s).wait_send()

            send_sib(arr, s).wait_send()
            send_sib(arr, sy).wait_send()


class ExpertTiles:
    def __init__(self, x_in, d_in, go, dx, wg, wu, wd, te, tk, tn, sg, xb, db, gob, dxb, wb, in_sem, out_sem, w_sem):
        self.te, self.tk, self.tn, self.sg = te, tk, tn, sg
        self.x_in, self.d_in, self.go, self.dx = x_in, d_in, go, dx
        self.w = (wg, wu, wd)
        self.xb, self.db, self.gob, self.dxb, self.wb = xb, db, gob, dxb, wb
        self.in_sem, self.out_sem, self.w_sem = in_sem, out_sem, w_sem

    def seg(self, ref, i, j):
        at = self.sg[i * HALF + j]
        return ref.at[at // 4, self.te[i], at % 4]

    def half(self, ref, i):
        return ref.at[pl.ds(pl.multiple_of(self.tk[i] * HALF, HALF), HALF), self.te[i], 0]

    def each(self, i, slot, act, moves, sem):
        @pl.when(self.tk[i] < 2)
        def _():
            for a, (hbm, buf, out) in enumerate(moves):
                ends = (buf.at[slot], self.half(hbm, i)) if out else (self.half(hbm, i), buf.at[slot])
                act(pltpu.make_async_copy(*ends, sem.at[a, slot, HALF]))

        for j in range(HALF):
            @pl.when((self.tk[i] == 2) & (j < self.tn[i]))
            def _():
                for a, (hbm, buf, out) in enumerate(moves):
                    ends = (buf.at[slot, j], self.seg(hbm, i, j)) if out else (self.seg(hbm, i, j), buf.at[slot, j])
                    act(pltpu.make_async_copy(*ends, sem.at[a, slot, j]))

    def load(self, i, slot, act):
        self.each(i, slot, act, ((self.x_in, self.xb, False), (self.d_in, self.db, False)), self.in_sem)

    def store(self, i, slot, act):
        self.each(i, slot, act, ((self.go, self.gob, True), (self.dx, self.dxb, True)), self.out_sem)

    def weights(self, e, p):
        return [pltpu.make_async_copy(src.at[e], self.wb.at[p, j], self.w_sem.at[p, j]) for j, src in enumerate(self.w)]

    def run(self, i, slot, p, fresh, dwb, dob, sgb, rank_ref, g_ref, dg_ref):
        rows = HALF * LEVEL_ROWS
        d_model = self.xb.shape[-1]
        one = pl.ds(self.te[i], 1)
        for j in range(HALF):
            at = self.sg[i * HALF + j]
            level = jnp.where(j < self.tn[i], at % 4, 8) * LEVEL_ROWS
            sgb[0, pl.ds(j, 1), :] = rank_ref[at // 4, one, :] - level.astype(F32)
            sgb[1, pl.ds(j, 1), :] = g_ref[at // 4, one, :]
        row = lax.broadcasted_iota(jnp.int32, (HALF, LEVEL_ROWS, LANES), 1)
        hit = sgb[0][:, None, :] == row.astype(F32)
        g_slot = jnp.sum(jnp.where(hit, sgb[1][:, None, :], 0.0), axis=2, keepdims=True).reshape(rows, 1)
        x = self.xb[slot].reshape(rows, d_model)
        h1 = dot_nt(x, self.wb[p, 0]).astype(BF16).astype(F32)
        h3 = dot_nt(x, self.wb[p, 1]).astype(BF16).astype(F32)
        sig = jax.nn.sigmoid(h1)
        silu = h1 * sig
        act = (silu * h3).astype(BF16)
        chunks = [slice(n, n + EXPERT_CHUNK) for n in range(0, d_model, EXPERT_CHUNK)]
        dg = jnp.zeros((rows, 1), F32)
        da = jnp.zeros((rows, act.shape[1]), F32)
        for cols in chunks:
            out = dot_nn(act, self.wb[p, 2, :, cols])
            dy = self.db[slot, :, :, cols].reshape(rows, EXPERT_CHUNK).astype(F32)
            dg = dg + jnp.sum(out * dy, axis=1, keepdims=True)
            self.gob[slot, :, :, cols] = (out * g_slot).astype(BF16).reshape(HALF, LEVEL_ROWS, EXPERT_CHUNK)
            do = (dy * g_slot).astype(BF16)
            dob[:, cols] = do
            da = da + dot_nt(do, self.wb[p, 2, :, cols])
        da = da.astype(BF16).astype(F32)
        dh1 = (da * h3 * sig * (1.0 + h1 * (1.0 - sig))).astype(BF16)
        dh3 = (da * silu).astype(BF16)
        for cols in chunks:
            dx = dot_nn(dh1, self.wb[p, 0, :, cols]) + dot_nn(dh3, self.wb[p, 1, :, cols])
            self.dxb[slot, :, :, cols] = dx.astype(BF16).reshape(HALF, LEVEL_ROWS, EXPERT_CHUNK)
        sgb[0] = jnp.sum(jnp.where(hit, dg.reshape(HALF, LEVEL_ROWS, 1), 0.0), axis=1)
        for j in range(HALF):
            dg_ref[self.sg[i * HALF + j] // 4, one, :] += sgb[0, pl.ds(j, 1), :]

        def add_dw(first):
            for cols in chunks:
                xc = self.xb[slot, :, :, cols].reshape(rows, EXPERT_CHUNK)
                for j, (left, right) in enumerate(((dh1, xc), (dh3, xc), (act, dob[:, cols]))):
                    part = dot_tn(left, right)
                    dwb[p, j, :, cols] = part if first else dwb[p, j, :, cols] + part

        @pl.when(fresh)
        def _():
            add_dw(True)

        @pl.when(jnp.logical_not(fresh))
        def _():
            add_dw(False)


def expert_kernel(cnt, x_hbm, d_hbm, wg_hbm, wu_hbm, wd_hbm, rank_ref, g_ref, go_hbm, dx_hbm, dwg_hbm, dwu_hbm, dwd_hbm, dg_ref,
                  te, tk, tn, sg, xb, db, gob, dxb, wb, dwb, dob, sgb, in_sem, out_sem, w_sem, dw_sem):
    local = wg_hbm.shape[0]
    levels = x_hbm.shape[2]
    blocks = x_hbm.shape[0]
    halves = blocks // HALF
    tiles = ExpertTiles(x_hbm, d_hbm, go_hbm, dx_hbm, wg_hbm, wu_hbm, wd_hbm, te, tk, tn, sg, xb, db, gob, dxb, wb, in_sem, out_sem, w_sem)

    def start(copy):
        copy.start()

    def wait(copy):
        copy.wait()

    def dw_out(e, p):
        return [pltpu.make_async_copy(dwb.at[p, j], dst.at[e], dw_sem.at[p, j]) for j, dst in enumerate((dwg_hbm, dwu_hbm, dwd_hbm))]

    te[0] = 0
    tk[0] = 0
    tn[0] = HALF
    for copy in tiles.weights(0, 0):
        copy.start()
    tiles.load(0, 0, start)
    dg_ref[...] = jnp.zeros(dg_ref.shape, F32)

    def add_expert(e, n):
        for h in range(halves):
            te[n + h] = e
            tk[n + h] = h
            tn[n + h] = HALF
            for j in range(HALF):
                sg[(n + h) * HALF + j] = (h * HALF + j) * 4
        n = n + halves

        def add_block(b, m):
            held = cnt[b, e]
            for level in range(1, levels):
                sg[n * HALF + m] = b * 4 + level
                m = m + jnp.where(held > level * LEVEL_ROWS, 1, 0)
            return m

        m = lax.fori_loop(0, blocks, add_block, 0)
        for j in range(HALF):
            sg[n * HALF + m + j] = 0
        extra = (m + HALF - 1) // HALF

        def add_tile(k, carry):
            te[n + k] = e
            tk[n + k] = 2
            tn[n + k] = jnp.minimum(m - k * HALF, HALF)
            return carry

        lax.fori_loop(0, extra, add_tile, 0)
        return n + extra

    count = lax.fori_loop(0, local, add_expert, 0)
    te[count] = local

    def step(i, carry):
        slot = i % 2
        e = te[i]
        p = e % 2
        fresh = (i == 0) | (te[jnp.maximum(i - 1, 0)] != e)
        last = te[i + 1] != e

        @pl.when(i + 1 < count)
        def _():
            tiles.load(i + 1, flipped(slot), start)

        @pl.when(fresh)
        def _():
            @pl.when(e + 1 < local)
            def _():
                for copy in tiles.weights(e + 1, flipped(p)):
                    copy.start()

            for copy in tiles.weights(e, p):
                copy.wait()

            @pl.when(e >= 2)
            def _():
                for copy in dw_out(e, p):
                    copy.wait()

        tiles.load(i, slot, wait)

        @pl.when(i >= 2)
        def _():
            tiles.store(i - 2, slot, wait)

        tiles.run(i, slot, p, fresh, dwb, dob, sgb, rank_ref, g_ref, dg_ref)
        tiles.store(i, slot, start)

        @pl.when(last)
        def _():
            for copy in dw_out(e, p):
                copy.start()

        return carry

    lax.fori_loop(0, count, step, 0)
    for p in PAIR:
        i = count - 2 + p
        tiles.store(i, i % 2, wait)
        for copy in dw_out(0, p):
            copy.wait()


def scatter_kernel(go_ref, dx_ref, uall_ref, rank_ref, dgb_ref, prob_ref, gown_ref, u_ref, dy_ref, wr_ref,
                   yo_ref, du_ref, dwr_ref,
                   slots, pbuf, acc, sib_out, sib_in, y_out, y_in, z_out, z_in, dg_in, dl_all, ubuf,
                   ld_sem, sib_ss, sib_rs, y_ss, y_rs, z_ss, z_rs, dg_ss, dg_rs, dl_ss, dl_rs, u_sem):
    y, c, z = position()
    me = block_of(y, c, z)
    ep_me = ep_of(y, c)
    ep_sib = ep_of(y, flipped(c))
    ep_y = ep_of(flipped(y), c)
    blocks, local, lanes = rank_ref.shape
    tok, d_model = u_ref.shape
    cap = pbuf.shape[1] // local
    experts = prob_ref.shape[0]

    def dg_copy(s, src):
        return pltpu.make_async_remote_copy(
            src_ref=dgb_ref.at[s], dst_ref=dg_in.at[src], send_sem=dg_ss.at[s], recv_sem=dg_rs.at[src],
            device_id=device_of(s), device_id_type=MESH)

    def dl_copy(s, src):
        return pltpu.make_async_remote_copy(
            src_ref=dl_all.at[src], dst_ref=dl_all.at[src], send_sem=dl_ss.at[s], recv_sem=dl_rs.at[src],
            device_id=device_of(s), device_id_type=MESH)

    def sib_copy(slot, arr, k):
        return pltpu.make_async_remote_copy(
            src_ref=sib_out.at[slot], dst_ref=sib_in.at[arr, k], send_sem=sib_ss.at[slot], recv_sem=sib_rs.at[arr, k],
            device_id={"ep": ep_sib, "etp": z}, device_id_type=MESH)

    def y_copy(arr, k):
        return pltpu.make_async_remote_copy(
            src_ref=y_out.at[arr, k], dst_ref=y_in.at[arr, k], send_sem=y_ss.at[arr, k], recv_sem=y_rs.at[arr, k],
            device_id={"ep": ep_y, "etp": z}, device_id_type=MESH)

    def z_copy(arr, k, slot, z_to):
        return pltpu.make_async_remote_copy(
            src_ref=z_out.at[arr, k], dst_ref=z_in.at[arr, slot], send_sem=z_ss.at[arr, k], recv_sem=z_rs.at[arr, slot],
            device_id={"ep": ep_me, "etp": z_to}, device_id_type=MESH)

    def plan(n):
        group = (n - 12) // 3
        rest = (n - 12) % 3
        mid = (n >= 12) & (n < 21)
        arr = jnp.where((n < 12) | (n == 23) | (mid & (rest == 0)), 0, 1)
        phase = jnp.where(n < 8, 1, jnp.where(n < 12, 2, jnp.where(n < 21, jnp.where(rest == 0, 3, 1), jnp.where(n < 23, 1, jnp.where(n == 23, 3, jnp.where(n < 28, 2, 3))))))
        sub = jnp.where(n < 8, n % 2, jnp.where(n < 21, rest - 1, n - 21))
        k = jnp.where(n < 8, n // 2, jnp.where(n < 12, n - 8, jnp.where(n < 21, group, jnp.where(n < 24, 3, n % 4))))
        to_sib = jnp.where(phase == 1, 1 - sub, jnp.where(phase == 2, 1, 0))
        other = jnp.where(phase == 1, 1, 0)
        core = swap(c, to_sib)
        col = swap(y, other)
        return arr, phase, k, to_sib, block_of(col, core, far_order(z, k))

    def start_load(n, slot):
        arr, phase, k, to_sib, s = plan(n)

        @pl.when(arr == 0)
        def _():
            pltpu.make_async_copy(go_ref.at[s], slots.at[slot], ld_sem.at[slot]).start()

        @pl.when(arr == 1)
        def _():
            pltpu.make_async_copy(dx_ref.at[s], slots.at[slot], ld_sem.at[slot]).start()

    start_load(0, 0)

    @pl.loop(1, blocks)
    def _(i):
        dg_copy((me + i) % blocks, me).start()

    dg_in[me] = dgb_ref[me]
    dwr_ref[...] = jnp.zeros(dwr_ref.shape, F32)

    def u_load(b):
        return pltpu.make_async_copy(uall_ref.at[b], ubuf.at[b % 2], u_sem.at[b % 2])

    @pl.loop(0, 32)
    def _(n):
        slot = n % 2
        arr, phase, k, to_sib, s = plan(n)

        @pl.when(n < 31)
        def _():
            start_load(n + 1, flipped(slot))

        pbuf[...] = one_hot_tokens(rank_ref[s][:, 0:tok], cap)
        pltpu.make_async_copy(go_ref.at[s], slots.at[slot], ld_sem.at[slot]).wait()

        @pl.loop(0, d_model // CHUNK)
        def _(m):
            cols = pl.ds(pl.multiple_of(m * CHUNK, CHUNK), CHUNK)
            acc[:, cols] = dot_nn(pbuf[...], slots[slot, :, cols])

        @pl.when(to_sib == 1)
        def _():
            idx = k + 4 * (phase - 1)
            out = idx % 2

            @pl.when((idx >= 2) | (arr == 1))
            def _():
                sib_copy(out, arr, idx).wait_send()

            sib_out[out] = acc[...].astype(BF16)
            sib_copy(out, arr, idx).start()

        @pl.when((phase == 1) & (to_sib == 0))
        def _():
            sib_copy(0, arr, k).wait_recv()
            y_out[arr, k] = (acc[...] + sib_in[arr, k].astype(F32)).astype(BF16)
            y_copy(arr, k).start()

        @pl.when(phase == 3)
        def _():
            sib_copy(0, arr, k + 4).wait_recv()
            y_copy(arr, k).wait_recv()
            acc[...] = acc[...] + sib_in[arr, k + 4].astype(F32) + y_in[arr, k].astype(F32)
            target = far_order(z, k)

            @pl.when(((target > z) & (z > 0)) | ((target < z) & (z < 3)) | ((target == z) & (z > 0)))
            def _():
                z_copy(arr, 0, target, z).wait_recv()
                acc[...] += z_in[arr, target].astype(F32)

            @pl.when((target == z) & (z < 3))
            def _():
                z_copy(arr, 0, 4, z).wait_recv()
                acc[...] += z_in[arr, 4].astype(F32)

            @pl.when(k < 3)
            def _():
                z_out[arr, k] = acc[...].astype(BF16)
                z_to = jnp.where(target > z, z + 1, z - 1)
                dst = jnp.where(target == z - 1, 4, target)
                z_copy(arr, k, dst, z_to).start()

            @pl.when((k == 3) & (arr == 0))
            def _():
                yo_ref[...] = (u_ref[...].astype(F32) + acc[...]).astype(BF16)

            @pl.when((k == 3) & (arr == 1))
            def _():
                dl3 = split3(dl_all[me][:, 0:tok])
                wr = wr_ref[...]
                router = dot_tn(dl3, jnp.concatenate([wr, wr, wr], axis=0))
                du_ref[...] = (dy_ref[...].astype(F32) + acc[...] + router).astype(BF16)

        @pl.when(n == 1)
        def _():
            @pl.loop(0, blocks)
            def _(b):
                @pl.when(b != me)
                def _():
                    dg_copy(me, b).wait_recv()

            d_gate = jnp.sum(dg_in[...].reshape(4, 4, local, lanes), axis=1).reshape(experts, lanes)
            d_prob = jnp.where(gown_ref[...] >= 0.0, d_gate, 0.0)
            prob = prob_ref[...]
            dl_all[me] = prob * (d_prob - jnp.sum(prob * d_prob, axis=0, keepdims=True))

            @pl.loop(1, blocks)
            def _(b):
                dl_copy((me + b) % blocks, me).start()

        @pl.when((n >= 15) & (n < 31))
        def _():
            u_load(n - 15).start()

        @pl.when(n >= 16)
        def _():
            b = n - 16

            @pl.when(b != me)
            def _():
                dl_copy(me, b).wait_recv()

            u_load(b).wait()
            part = dot_nn(split3(dl_all[b][:, 0:tok]), ubuf[b % 2])
            dwr_ref[...] += part[0:experts] + part[experts:2 * experts] + part[2 * experts:3 * experts]

    for out in PAIR:
        sib_copy(out, 0, 0).wait_send()

    @pl.loop(0, 4)
    def _(k):
        for arr in PAIR:
            y_copy(arr, k).wait_send()

            @pl.when(k < 3)
            def _():
                z_copy(arr, k, 0, z).wait_send()

    @pl.loop(0, blocks)
    def _(b):
        @pl.when(b != me)
        def _():
            dg_copy(b, me).wait_send()
            dl_copy(b, me).wait_send()


def solution(mesh):
    ep_size = mesh.shape["ep"]
    etp_size = mesh.shape["etp"]
    blocks = ep_size * etp_size
    tok_spec = P(("dp", "ep", "etp"), None)
    col_spec = P("ep", None, "etp")
    row_spec = P("ep", "etp", None)
    in_specs = (tok_spec, tok_spec, tok_spec, P(None, None), col_spec, col_spec, row_spec)
    out_specs = (tok_spec, tok_spec, P(("dp", "ep"), None, "etp"), P(("dp", "ep"), None, "etp"), P(("dp", "ep"), "etp", None), P("dp", None))
    any_spec = pl.BlockSpec(memory_space=pl.ANY)
    vmem = pl.BlockSpec(memory_space=pltpu.VMEM)
    dma = pltpu.SemaphoreType.DMA

    def device_step(u_loc, dy_loc, ids_loc, w_router, w_gate, w_up, w_down):
        tok, d_model = u_loc.shape
        top_k = ids_loc.shape[1]
        experts = w_router.shape[1]
        local = w_gate.shape[0]
        ffn = w_gate.shape[2]
        cap = 96
        slots = local * cap
        ids_t = ids_loc.T
        wr_t = w_router.T
        wg_t = jnp.swapaxes(w_gate, 1, 2)
        wu_t = jnp.swapaxes(w_up, 1, 2)

        levels = cap // LEVEL_ROWS
        tile_shape = jax.ShapeDtypeStruct((blocks, local, levels, LEVEL_ROWS, d_model), BF16)
        dw_shape = jax.ShapeDtypeStruct((local, ffn, d_model), F32)
        meta_shape = jax.ShapeDtypeStruct((blocks, local, LANES), F32)
        own_shape = jax.ShapeDtypeStruct((experts, LANES), F32)
        tile_buf = pltpu.VMEM((2, HALF, LEVEL_ROWS, d_model), BF16)
        weight_buf = pltpu.VMEM((2, 3, ffn, d_model), BF16)
        x_slots, d_slots, u_all, rank, gate, prob, g_own, counts = pl.pallas_call(
            gather_kernel,
            name="gather",
            out_shape=(tile_shape, tile_shape, jax.ShapeDtypeStruct((blocks, tok, d_model), BF16), meta_shape, meta_shape, own_shape, own_shape,
                       jax.ShapeDtypeStruct((blocks, 128), jnp.int32)),
            in_specs=[any_spec, any_spec, vmem, vmem],
            out_specs=(any_spec, any_spec, any_spec, vmem, vmem, vmem, vmem, vmem),
            scratch_shapes=[
                pltpu.VMEM((2, blocks, tok, d_model), BF16),
                pltpu.VMEM((slots, tok), BF16),
                pltpu.VMEM((2, local, levels, LEVEL_ROWS, d_model), BF16),
                dma((2,)), dma((2, blocks, 4)), dma((2, blocks)), dma((2, blocks)), dma((blocks,)), dma((blocks,)), dma((2,)), dma((blocks,)),
            ],
            compiler_params=pltpu.CompilerParams(has_side_effects=True, vmem_limit_bytes=VMEM_LIMIT),
        )(u_loc, dy_loc, ids_t, wr_t)

        max_tiles = local * levels * (blocks // HALF) + 8
        smem_list = pltpu.SMEM((max_tiles,), jnp.int32)
        smem = pl.BlockSpec(memory_space=pltpu.SMEM)
        go, dx, dwg, dwu, dwd, dg_blocks = pl.pallas_call(
            expert_kernel,
            name="experts",
            out_shape=(tile_shape, tile_shape, dw_shape, dw_shape, dw_shape, meta_shape),
            in_specs=[smem] + [any_spec] * 5 + [vmem] * 2,
            out_specs=(any_spec,) * 5 + (vmem,),
            scratch_shapes=[
                smem_list, smem_list, smem_list, pltpu.SMEM((max_tiles * HALF,), jnp.int32), tile_buf, tile_buf, tile_buf, tile_buf, weight_buf,
                pltpu.VMEM((2, 3, ffn, d_model), F32),
                pltpu.VMEM((HALF * LEVEL_ROWS, d_model), BF16),
                pltpu.VMEM((2, HALF, LANES), F32),
                dma((2, 2, HALF + 1)), dma((2, 2, HALF + 1)), dma((2, 3)), dma((2, 3)),
            ],
            input_output_aliases={1: 0, 2: 1},
            compiler_params=pltpu.CompilerParams(vmem_limit_bytes=VMEM_LIMIT),
        )(counts, x_slots, d_slots, wg_t, wu_t, w_down, rank, gate)

        slot_shape = (blocks, slots, d_model)
        y_loc, du_loc, dwr_t = pl.pallas_call(
            scatter_kernel,
            name="scatter",
            out_shape=(jax.ShapeDtypeStruct((tok, d_model), BF16), jax.ShapeDtypeStruct((tok, d_model), BF16), jax.ShapeDtypeStruct((experts, d_model), F32)),
            in_specs=[any_spec, any_spec, any_spec] + [vmem] * 7,
            out_specs=(vmem, vmem, vmem),
            scratch_shapes=[
                pltpu.VMEM((2, slots, d_model), BF16),
                pltpu.VMEM((tok, slots), BF16),
                pltpu.VMEM((tok, d_model), F32),
                pltpu.VMEM((2, tok, d_model), BF16),
                pltpu.VMEM((2, 8, tok, d_model), BF16),
                pltpu.VMEM((2, 4, tok, d_model), BF16),
                pltpu.VMEM((2, 4, tok, d_model), BF16),
                pltpu.VMEM((2, 3, tok, d_model), BF16),
                pltpu.VMEM((2, 5, tok, d_model), BF16),
                pltpu.VMEM((blocks, local, LANES), F32),
                pltpu.VMEM((blocks, experts, LANES), F32),
                pltpu.VMEM((2, tok, d_model), BF16),
                dma((2,)), dma((2,)), dma((2, 8)), dma((2, 4)), dma((2, 4)), dma((2, 3)), dma((2, 5)),
                dma((blocks,)), dma((blocks,)), dma((blocks,)), dma((blocks,)), dma((2,)),
            ],
            compiler_params=pltpu.CompilerParams(has_side_effects=True, vmem_limit_bytes=VMEM_LIMIT),
        )(go.reshape(slot_shape), dx.reshape(slot_shape), u_all, rank, dg_blocks, prob, g_own, u_loc, dy_loc, wr_t)

        dw_gate = jnp.swapaxes(dwg, 1, 2)
        dw_up = jnp.swapaxes(dwu, 1, 2)
        return y_loc, du_loc, dw_gate, dw_up, dwd, dwr_t.T

    return jax.shard_map(device_step, mesh=mesh, in_specs=in_specs, out_specs=out_specs, check_vma=False)
```
